256 devices in a mesh: tensor: 8 (over z), expert: 2 (over core), dp: 16 (over y, x).
Axes of the slice: x: 4, y: 4, z: 8, core: 2. Of those that a mesh axis runs over, the one named last changes fastest.
Arguments:
- tokens: bfloat16 [4096, 2048], P(('expert', 'dp')), may hold values from -6 to 6
- tangent: bfloat16 [4096, 2048], P(('expert', 'dp')), may hold values from -6 to 6
- cotangent: bfloat16 [4096, 2048], P(('expert', 'dp')), may hold values from -0.59765625 to 0.59765625
- expert_ids: int32 [4096, 8], P(('expert', 'dp')), may hold values from 0 to 15, all different within a row; in each aligned block of 128 rows (0 to 127, 128 to 255, ...) at most 96 rows name the same one
- gates: float32 [4096, 8], P(('expert', 'dp')), may hold values from 0.1 to 1
- w_in: bfloat16 [16, 2, 768, 2048], P(('tensor', 'expert'), None, None, 'dp'), may hold values from -0.125 to 0.125
- v_in: bfloat16 [16, 2, 768, 2048], P(('tensor', 'expert'), None, None, 'dp'), may hold values from -0.125 to 0.125
- w_out: bfloat16 [16, 768, 2048], P(('tensor', 'expert'), None, 'dp'), may hold values from -0.21875 to 0.21875
- v_out: bfloat16 [16, 768, 2048], P(('tensor', 'expert'), None, 'dp'), may hold values from -0.21875 to 0.21875
Outputs:
- hvp_tokens: float32 [4096, 2048], P(('expert', 'dp'))
- hvp_in: float32 [16, 2, 768, 2048], P(('tensor', 'expert'), None, None, 'dp')
- hvp_out: float32 [16, 768, 2048], P(('tensor', 'expert'), None, 'dp')
The draws below stay inside these ranges and needn't reach their ends.
Inputs may be any that keep to these rules, and one draw needn't show every extreme that they name: `expert_ids`: each token names 8 different experts; among the tokens of one block of 128 no expert is named more than 96 times, and some expert reaches 96 in some blocks.
All inputs are finite; a program needn't handle non-finite values.
Results may differ from the reference program's by a relative error of at most 0.013.
Values may be sent and summed in bfloat16 or wider, within the bound.
A program may use at most 128 MiB of HBM per device.

```python
import math
import jax
import jax.numpy as jnp
import numpy as np
from jax import lax

D = 2048
FF = 768
TOPK = 8
TOK_DEV = 128
EXPERTS = 16
CAP = 96
TOKENS = 4096
N_EXPERT = 2
N_DP = 16


def level_of(rng, extent, pieces, least, high):
    def one(axis_at, blocks):
        draws = jax.random.uniform(jax.random.fold_in(jax.random.fold_in(rng, 6), axis_at), (blocks,), jnp.float32, least / len(pieces), high / len(pieces))
        return jnp.repeat(jnp.exp(draws), extent[axis_at] // blocks).reshape((-1,) + (1,) * (len(extent) - axis_at - 1))

    level = one(*pieces[0])
    for cut in pieces[1:]:
        level = level * one(*cut)
    return level


def routed_block(rng, own, number, rows, number_of, top, reach, slope):
    order = jax.random.permutation(rng, number_of)
    heavy_load, ordinary = shares(number_of, rows * top, reach, slope, True), shares(number_of, rows * top, reach, slope, False)
    places = jnp.arange(number_of)

    def named(tallies, turn):
        used = int((tallies > 0).sum())
        fixed = max(1, used // 4)
        passed = fixed + (places - fixed + turn * (used - fixed)) % max(1, number_of - fixed)
        return jnp.zeros((number_of,), jnp.int32).at[order[jnp.where(places < fixed, places, passed)]].set(jnp.asarray(tallies, jnp.int32))

    tallies = jnp.where(number % 4 == 0, named(heavy_load, number // 4), named(ordinary, number - number // 4 - 1))
    mixed = jax.random.permutation(jax.random.fold_in(own, 3), number_of)
    source_of, receiver = mixed[0:number_of // 2 * 2:2], mixed[1:number_of // 2 * 2:2]
    room = jnp.minimum(tallies[source_of] - 1, reach - tallies[receiver]) // 2
    room = jnp.where((source_of == order[0]) | (receiver == order[0]) | (tallies[receiver] == 0), 0, jnp.maximum(room, 0))
    passed = jax.random.randint(jax.random.fold_in(own, 4), (number_of // 2,), 0, 1 << 20) % (room + 1)
    tallies = tallies.at[source_of].add(-passed).at[receiver].add(passed)
    items = jnp.searchsorted(jnp.cumsum(tallies), jnp.arange(rows * top), side="right").astype(jnp.int32)
    table = items.reshape(top, rows).T
    table = table[jax.random.permutation(jax.random.fold_in(own, 1), rows)]
    turn = jax.random.randint(jax.random.fold_in(own, 2), (rows, 1), 0, top)
    return jnp.take_along_axis(table, (jnp.arange(top)[None, :] + turn) % top, axis=1)


def shares(amount, total, reach, lean, full):
    portions = [(1 << 20) // math.isqrt(standing ** lean) + 1 for standing in range(1, amount + 1)]
    largest = reach if full else min(reach, max(-(-total // amount), total * portions[0] // sum(portions)))
    least = 1 if total - largest >= amount - 1 else 0
    holding, rest = [largest] + [least] * (amount - 1), total - largest - least * (amount - 1)
    while rest > 0:
        free = [i for i in range(1, amount) if holding[i] < largest] or [i for i in range(1, amount) if holding[i] < reach]
        mass, budget = sum([portions[i] for i in free]), rest
        for i in free:
            addition = min(reach - holding[i], max(1, budget * portions[i] // mass), rest)
            holding[i] = holding[i] + addition
            rest = rest - addition
    return np.array(holding)


def scatter_about(rng, extent, width, bound, split=(), kind=jnp.bfloat16):
    factor_of = level_of(rng, extent, split, -0.22, 0.18) if split else 1.0
    entries = jax.random.normal(rng, extent, jnp.float32) * width * factor_of
    return jnp.minimum(jnp.maximum(entries, -bound), bound).astype(kind)


def setup_inputs(seed: int = 0) -> dict:
    key_of = jax.random.split(jax.random.key(seed), 10)
    tokens = scatter_about(key_of[0], (TOKENS, D), 1.0, 6.0, ((0, 32),))
    tangent = scatter_about(key_of[1], (TOKENS, D), 1.0, 6.0, ((0, 32),))
    cotangent = scatter_about(key_of[2], (TOKENS, D), 0.1, 0.59765625, ((0, 32),))
    expert_ids_keys = jax.random.split(jax.random.fold_in(key_of[3], 1), TOKENS // TOK_DEV)
    expert_ids_turns = jax.random.permutation(jax.random.fold_in(key_of[3], 3), TOKENS // TOK_DEV)
    expert_ids = jax.vmap(lambda own, number: routed_block(jax.random.fold_in(key_of[3], 2), own, number, TOK_DEV, EXPERTS, TOPK, CAP, 2))(expert_ids_keys, expert_ids_turns).reshape((TOKENS, TOPK))
    gates = jnp.clip(jnp.exp(math.log(1.0) - 2.3025851 * jax.random.uniform(key_of[4], (TOKENS, TOPK), jnp.float32) ** level_of(key_of[4], (TOKENS, TOPK), ((0, 32),), -0.2, 0.2)), 0.1, 1.0)
    w_in = scatter_about(key_of[5], (EXPERTS, 2, FF, D), D ** -0.5, 0.125, ((0, 16), (3, 16)))
    v_in = scatter_about(key_of[6], (EXPERTS, 2, FF, D), D ** -0.5, 0.125, ((0, 16), (3, 16)))
    w_out = scatter_about(key_of[7], (EXPERTS, FF, D), FF ** -0.5, 0.21875, ((0, 16), (2, 16)))
    v_out = scatter_about(key_of[8], (EXPERTS, FF, D), FF ** -0.5, 0.21875, ((0, 16), (2, 16)))
    return {"tokens": tokens, "tangent": tangent, "cotangent": cotangent, "expert_ids": expert_ids, "gates": gates, "w_in": w_in, "v_in": v_in, "w_out": w_out, "v_out": v_out}


def rounded(value):
    return lax.optimization_barrier(value.astype(jnp.bfloat16)).astype(jnp.float32)


def reference(tokens, tangent, cotangent, expert_ids, gates, w_in, v_in, w_out, v_out):
    blocks = N_EXPERT * N_DP
    pairs = TOK_DEV * TOPK
    picks = expert_ids.reshape(blocks, pairs).astype(jnp.int32)
    onehot = (picks[:, :, None] == jnp.arange(EXPERTS, dtype=jnp.int32)[None, None, :]).astype(jnp.int32)
    running = jnp.cumsum(onehot, axis=1) - 1
    slots = jnp.sum(onehot * running, axis=2).astype(jnp.int32)
    block_ids = jnp.broadcast_to(jnp.arange(blocks, dtype=jnp.int32)[:, None], (blocks, pairs))
    replica = block_ids % N_DP
    source = block_ids // N_DP
    token_ids = block_ids * TOK_DEV + (jnp.arange(pairs, dtype=jnp.int32) // TOPK)[None, :]
    shape = (N_DP, EXPERTS, N_EXPERT, CAP)
    tables = jnp.full(shape, TOKENS, jnp.int32).at[replica, picks, source, slots].set(token_ids)
    scales = jnp.zeros(shape, jnp.float32).at[replica, picks, source, slots].set(gates.reshape(blocks, pairs))
    zero_row = jnp.zeros((1, D), jnp.bfloat16)
    pad_x = jnp.concatenate([tokens, zero_row], axis=0)
    pad_u = jnp.concatenate([tangent, zero_row], axis=0)
    pad_c = jnp.concatenate([cotangent, zero_row], axis=0)

    def one_expert(carry, expert):
        index = tables[:, expert].reshape(N_DP, -1)
        scale = scales[:, expert].reshape(N_DP, -1)
        rows_x = pad_x[index].astype(jnp.float32)
        rows_u = pad_u[index].astype(jnp.float32)
        rows_dy = rounded(scale[:, :, None] * pad_c[index].astype(jnp.float32))
        w_first = w_in[expert].astype(jnp.float32)
        v_first = v_in[expert].astype(jnp.float32)
        w_second = w_out[expert].astype(jnp.float32)
        v_second = v_out[expert].astype(jnp.float32)
        pre = jnp.einsum("prd,gfd->prgf", rows_x, w_first)
        pre_dot = jnp.einsum("prd,gfd->prgf", rows_u, w_first) + jnp.einsum("prd,gfd->prgf", rows_x, v_first)
        gate_pre, up_val = pre[:, :, 0], pre[:, :, 1]
        gate_dot, up_dot = pre_dot[:, :, 0], pre_dot[:, :, 1]
        back = jnp.einsum("prd,fd->prf", rows_dy, w_second)
        back_dot = jnp.einsum("prd,fd->prf", rows_dy, v_second)
        sigma = jax.nn.sigmoid(gate_pre)
        silu_val = gate_pre * sigma
        first = sigma * (1.0 + gate_pre * (1.0 - sigma))
        second = sigma * (1.0 - sigma) * (2.0 + gate_pre * (1.0 - 2.0 * sigma))
        grad_a = back * up_val * first
        grad_b = back * silu_val
        tang_a = back_dot * up_val * first + back * up_dot * first + back * up_val * second * gate_dot
        tang_b = back_dot * silu_val + back * first * gate_dot
        grads = rounded(jnp.stack([grad_a, grad_b], axis=2))
        tangs = rounded(jnp.stack([tang_a, tang_b], axis=2))
        hidden_dot = rounded(first * gate_dot * up_val + silu_val * up_dot)
        partial_value = jnp.einsum("prgf,gfd->prd", tangs, w_first) + jnp.einsum("prgf,gfd->prd", grads, v_first)
        partial_value = rounded(partial_value)
        carry = carry.at[index.reshape(-1)].add(partial_value.reshape(-1, D))
        part_in = jnp.einsum("prd,prgf->pgfd", rows_u, grads) + jnp.einsum("prd,prgf->pgfd", rows_x, tangs)
        part_out = jnp.einsum("prf,prd->pfd", hidden_dot, rows_dy)
        return carry, (jnp.sum(rounded(part_in), axis=0), jnp.sum(rounded(part_out), axis=0))

    start = jnp.zeros((TOKENS + 1, D), jnp.float32)
    total, results = lax.scan(one_expert, start, jnp.arange(EXPERTS, dtype=jnp.int32))
    return total[:TOKENS], results[0], results[1]
```

```python
import functools

import jax
import jax.numpy as jnp
from jax import lax
from jax.experimental import pallas as pl
from jax.experimental.pallas import tpu as pltpu
from jax.sharding import PartitionSpec as P

MESH = pl.DeviceIdType.MESH
F32 = jnp.float32
BF16 = jnp.bfloat16
SIDE = 4
NT = (((1,), (1,)), ((), ()))
NN = (((1,), (0,)), ((), ()))


def mm(a, b, dims=NN):
    return lax.dot_general(a, b, dims, preferred_element_type=F32)


def kernel(
    n_z, ids_ref, gates_ref, tok_ref, tan_ref, cot_ref, wi_ref, vi_ref, wo_ref, vo_ref,
    out_tok, out_in, out_out,
    W, X, G, C, S, ST, H, acc, Pown, PDs, PDr, xs, xopp, xr, xropp, ys, yopp, yr, yropp, R, OUT, Zs, Zr, Zf,
    loc, wa_s, wa_r, wy_s, wy_r, wf_s, wf_r, xh_s, xh_r, xf_s, xf_r, g_s, g_r, gd, dd_s, dd_r, pd_s, pd_r,
    xo_s, xo_r, xp_s, xp_r, yo_s, yo_r, yp_s, yp_r, ra_s, ra_r, z1_s, z1_r, z2_s, z2_r,
):
    t = lax.axis_index("tensor")
    e = lax.axis_index("expert")
    p = lax.axis_index("dp")
    y, x = p // SIDE, p % SIDE
    tok = tok_ref.shape[0]
    half = tok // 2
    lanes = wi_ref.shape[-1]
    q = W.shape[1]
    width = W.shape[2]
    part = width // SIDE

    def at_x(d):
        return lax.rem(x + d, SIDE)

    def at_y(d):
        return lax.rem(y + d, SIDE)

    def dev_x(d):
        return (t, e, y * SIDE + at_x(d))

    def dev_y(d):
        return (t, e, at_y(d) * SIDE + x)

    def dev_z(d):
        return (lax.rem(t + d, n_z), e, p)

    partner = (t, 1 - e, p)
    pending = []

    def send(src, dst, ssem, rsem, dev):
        copy = pltpu.make_async_remote_copy(
            src_ref=src, dst_ref=dst, send_sem=ssem, recv_sem=rsem, device_id=dev, device_id_type=MESH
        )
        copy.start()
        pending.append(copy)

    def got(dst, ssem, rsem):
        pltpu.make_async_remote_copy(
            src_ref=dst, dst_ref=dst, send_sem=ssem, recv_sem=rsem, device_id=partner, device_id_type=MESH
        ).wait_recv()

    barrier = pltpu.get_barrier_semaphore()
    peers = [partner] + [dev_x(d) for d in (1, 2, 3)] + [dev_y(d) for d in (1, 3)] + [dev_z(d) for d in range(1, n_z)]
    for peer in peers:
        pl.semaphore_signal(barrier, inc=1, device_id=peer, device_id_type=MESH)

    def slab(yy, xx):
        return pl.ds(pl.multiple_of((yy * SIDE + xx) * lanes, lanes), lanes)

    def rows(k):
        return pl.ds(pl.multiple_of(k * q, q), q)

    mine = [
        pltpu.make_async_copy(tok_ref, X.at[0, x, e], loc.at[0]),
        pltpu.make_async_copy(tan_ref, X.at[1, x, e], loc.at[1]),
        pltpu.make_async_copy(cot_ref, X.at[2, x, e], loc.at[2]),
        pltpu.make_async_copy(wi_ref.at[:, rows(x), :], W.at[0:2, :, slab(y, x)], loc.at[3]),
        pltpu.make_async_copy(vi_ref.at[:, rows(x), :], W.at[2:4, :, slab(y, x)], loc.at[4]),
        pltpu.make_async_copy(wo_ref.at[rows(x), :], W.at[4, :, slab(y, x)], loc.at[5]),
        pltpu.make_async_copy(vo_ref.at[rows(x), :], W.at[5, :, slab(y, x)], loc.at[6]),
    ]
    for copy in mine:
        copy.start()
    ids, gates = ids_ref[...], gates_ref[...]
    for r in range(2):
        G[e, x, pl.ds(r, 1), :] = jnp.sum(jnp.where(ids == 2 * t + r, gates, 0.0), axis=0, keepdims=True)
    pl.semaphore_wait(barrier, len(peers))

    for k, d in enumerate((1, 3, 2)):
        dst = slab(y, x)
        for i, (src, to) in enumerate(
            (
                (wi_ref.at[:, rows(at_x(d)), :], W.at[0:2, :, dst]),
                (vi_ref.at[:, rows(at_x(d)), :], W.at[2:4, :, dst]),
                (wo_ref.at[rows(at_x(d)), :], W.at[4, :, dst]),
                (vo_ref.at[rows(at_x(d)), :], W.at[5, :, dst]),
            )
        ):
            send(src, to, wa_s.at[k, i], wa_r.at[k, i], dev_x(d))
    for k, d in enumerate((1, 3, 2)):
        send(G.at[e, x], G.at[e, x], g_s.at[k], g_r.at[k], dev_x(d))
    for copy in mine:
        copy.wait()

    def xhalf(a, core, h):
        return X.at[:, a, core, pl.ds(h * half, half), :]

    send(xhalf(x, e, 0), xhalf(x, e, 0), xh_s.at[0, 0], xh_r.at[0, 0], dev_x(1))
    send(xhalf(x, e, 1), xhalf(x, e, 1), xh_s.at[1, 1], xh_r.at[1, 1], dev_x(3))
    send(xhalf(x, e, 1), xhalf(x, e, 1), xh_s.at[0, 1], xh_r.at[0, 1], dev_x(1))
    send(xhalf(x, e, 0), xhalf(x, e, 0), xh_s.at[1, 0], xh_r.at[1, 0], dev_x(3))
    for h in range(2):
        send(xhalf(x, e, h), xhalf(x, e, h), dd_s.at[0, h], dd_r.at[0, h], partner)

    def wslab(yy, d):
        return W.at[:, :, slab(yy, at_x(SIDE - d))]

    def whalf(yy, d, h):
        return W.at[3 * h : 3 * h + 3, :, slab(yy, at_x(SIDE - d))]

    order = (0, 1, 3, 2)
    for k, d in enumerate(order):
        if d:
            i = (1, 3, 2).index(d)
            src = slab(y, at_x(SIDE - d))
            for j, to in enumerate((W.at[0:2, :, src], W.at[2:4, :, src], W.at[4, :, src], W.at[5, :, src])):
                got(to, wa_s.at[i, j], wa_r.at[i, j])
        send(wslab(y, d), wslab(y, d), wy_s.at[0, k], wy_r.at[0, k], dev_y(1))
        send(wslab(y, d), wslab(y, d), wy_s.at[1, k], wy_r.at[1, k], dev_y(3))
    for k, d in enumerate(order):
        got(wslab(at_y(3), d), wy_s.at[0, k], wy_r.at[0, k])
        send(whalf(at_y(3), d, 0), whalf(at_y(3), d, 0), wf_s.at[0, k], wf_r.at[0, k], dev_y(1))
        got(wslab(at_y(1), d), wy_s.at[1, k], wy_r.at[1, k])
        send(whalf(at_y(1), d, 1), whalf(at_y(1), d, 1), wf_s.at[1, k], wf_r.at[1, k], dev_y(3))

    for k, d in enumerate((1, 3, 2)):
        src = at_x(SIDE - d)
        got(G.at[e, src], g_s.at[k], g_r.at[k])
    send(G.at[e], G.at[e], gd.at[0], gd.at[1], partner)

    got(xhalf(at_x(3), e, 0), xh_s.at[0, 0], xh_r.at[0, 0])
    send(xhalf(at_x(3), e, 0), xhalf(at_x(3), e, 0), xf_s.at[0], xf_r.at[0], dev_x(1))
    send(xhalf(at_x(3), e, 0), xhalf(at_x(3), e, 0), dd_s.at[1, 0], dd_r.at[1, 0], partner)
    got(xhalf(at_x(1), e, 1), xh_s.at[1, 1], xh_r.at[1, 1])
    send(xhalf(at_x(1), e, 1), xhalf(at_x(1), e, 1), xf_s.at[1], xf_r.at[1], dev_x(3))
    send(xhalf(at_x(1), e, 1), xhalf(at_x(1), e, 1), dd_s.at[3, 1], dd_r.at[3, 1], partner)

    for k, d in enumerate(order):
        got(whalf(at_y(2), d, 0), wf_s.at[0, k], wf_r.at[0, k])
        got(whalf(at_y(2), d, 1), wf_s.at[1, k], wf_r.at[1, k])
    got(G.at[1 - e], gd.at[0], gd.at[1])

    n_acc = acc.shape[1]
    cut = n_acc // 2
    step = 32

    def group(a, rel, first):
        def both(i, cols=slice(None)):
            v = X[i, a, :, :, cols]
            return v.reshape(2 * tok, v.shape[-1])

        C[0 : 2 * q, :] = mm(W[0:2].reshape(2 * q, width), both(0), NT)
        C[2 * q : 4 * q, :] = mm(W[2:4].reshape(2 * q, width), both(0), NT)
        C[4 * q : 6 * q, :] = mm(W[0:2].reshape(2 * q, width), both(1), NT)
        C[6 * q : 8 * q, :] = mm(W[4:6].reshape(2 * q, width), both(2), NT)
        gate = jnp.concatenate([G[0, a, pl.ds(e, 1), :], G[1, a, pl.ds(e, 1), :]], axis=1)

        def rows_of(i, carry):
            at = pl.multiple_of(i * step, step)

            def c(k):
                return C[pl.ds(k * q + at, step), :]

            pre, up = c(0), c(1)
            pre_dot, up_dot = c(4) + c(2), c(5) + c(3)
            g, g_dot = c(6) * gate, c(7) * gate
            sigma = jax.nn.sigmoid(pre)
            rest = 1.0 - sigma
            s0 = pre * sigma
            s1 = sigma * (1.0 + pre * rest)
            s2 = sigma * rest * (2.0 + pre * (1.0 - 2.0 * sigma))
            S[pl.ds(at, step), :] = (
                g_dot * up * s1 + g * up_dot * s1 + g * up * s2 * pre_dot
            ).astype(BF16)
            S[pl.ds(q + at, step), :] = (g_dot * s0 + g * s1 * pre_dot).astype(BF16)
            S[pl.ds(2 * q + at, step), :] = (g * up * s1).astype(BF16)
            S[pl.ds(3 * q + at, step), :] = (g * s0).astype(BF16)
            H[pl.ds(at, step), :] = ((s1 * pre_dot * up + s0 * up_dot) * gate).astype(BF16)
            return carry

        lax.fori_loop(0, q // step, rows_of, 0)
        ST[...] = S[...].T

        def columns(n, carry):
            cols = pl.ds(pl.multiple_of(n * part, part), part)
            value = mm(ST[...], W[0:4, :, cols].reshape(4 * q, part))
            for core in range(2):

                @pl.when(e == core)
                def _():
                    Pown[rel, :, cols] = value[core * tok : (core + 1) * tok]
                    PDs[rel, :, cols] = value[(1 - core) * tok : (2 - core) * tok].astype(BF16)

            w_in = mm(S[2 * q : 4 * q, :], both(1, cols)) + mm(S[0 : 2 * q, :], both(0, cols))
            w_out = mm(H[...], both(2, cols))
            if first:
                acc[n, 0 : 2 * q, :] = w_in
                acc[n, 2 * q : 3 * q, :] = w_out
            else:
                acc[n, 0 : 2 * q, :] += w_in
                acc[n, 2 * q : 3 * q, :] += w_out
            return carry

        lax.fori_loop(0, SIDE, columns, 0)
        send(PDs.at[rel], PDr.at[rel], pd_s.at[rel], pd_r.at[rel], partner)

    def summed(rel, h):
        at = pl.ds(h * half, half)
        return Pown[rel, at, :] + PDr[rel, at, :].astype(F32)

    for h in range(2):
        got(xhalf(x, 1 - e, h), dd_s.at[0, h], dd_r.at[0, h])
    group(x, 0, True)

    got(xhalf(at_x(3), e, 1), xh_s.at[0, 1], xh_r.at[0, 1])
    send(xhalf(at_x(3), e, 1), xhalf(at_x(3), e, 1), dd_s.at[1, 1], dd_r.at[1, 1], partner)
    got(xhalf(at_x(1), e, 0), xh_s.at[1, 0], xh_r.at[1, 0])
    send(xhalf(at_x(1), e, 0), xhalf(at_x(1), e, 0), dd_s.at[3, 0], dd_r.at[3, 0], partner)
    for h in range(2):
        got(xhalf(at_x(3), 1 - e, h), dd_s.at[1, h], dd_r.at[1, h])
    group(at_x(3), 1, False)

    got(xhalf(at_x(2), e, 0), xf_s.at[0], xf_r.at[0])
    send(xhalf(at_x(2), e, 0), xhalf(at_x(2), e, 0), dd_s.at[2, 0], dd_r.at[2, 0], partner)
    got(xhalf(at_x(2), e, 1), xf_s.at[1], xf_r.at[1])
    send(xhalf(at_x(2), e, 1), xhalf(at_x(2), e, 1), dd_s.at[2, 1], dd_r.at[2, 1], partner)
    for h in range(2):
        got(xhalf(at_x(1), 1 - e, h), dd_s.at[3, h], dd_r.at[3, h])
    group(at_x(1), 3, False)

    for h in range(2):
        got(xhalf(at_x(2), 1 - e, h), dd_s.at[2, h], dd_r.at[2, h])
    group(at_x(2), 2, False)

    def acc_half(k, h):
        return acc[k, h * cut : (h + 1) * cut, :]

    for h in range(2):
        yopp[h] = acc_half(at_y(2), h).astype(BF16)
        send(yopp.at[h], yropp.at[h], yo_s.at[h], yo_r.at[h], dev_y(1 + 2 * h))
    ys[0, 1] = acc_half(at_y(1), 1).astype(BF16)
    send(ys.at[0, 1], yr.at[0, 1], yp_s.at[0, 1], yp_r.at[0, 1], dev_y(1))
    ys[1, 0] = acc_half(at_y(3), 0).astype(BF16)
    send(ys.at[1, 0], yr.at[1, 0], yp_s.at[1, 0], yp_r.at[1, 0], dev_y(3))

    for rel in (0, 1, 3, 2):
        got(PDr.at[rel], pd_s.at[rel], pd_r.at[rel])
    for h in range(2):
        xopp[h] = summed(2, h).astype(BF16)
        send(xopp.at[h], xropp.at[h], xo_s.at[h], xo_r.at[h], dev_x(1 + 2 * h))
    xs[0, 1] = summed(3, 1).astype(BF16)
    send(xs.at[0, 1], xr.at[0, 1], xp_s.at[0, 1], xp_r.at[0, 1], dev_x(1))
    xs[1, 0] = summed(1, 0).astype(BF16)
    send(xs.at[1, 0], xr.at[1, 0], xp_s.at[1, 0], xp_r.at[1, 0], dev_x(3))

    got(xropp.at[0], xo_s.at[0], xo_r.at[0])
    xs[0, 0] = (summed(3, 0) + xropp[0].astype(F32)).astype(BF16)
    send(xs.at[0, 0], xr.at[0, 0], xp_s.at[0, 0], xp_r.at[0, 0], dev_x(1))
    got(xropp.at[1], xo_s.at[1], xo_r.at[1])
    xs[1, 1] = (summed(1, 1) + xropp[1].astype(F32)).astype(BF16)
    send(xs.at[1, 1], xr.at[1, 1], xp_s.at[1, 1], xp_r.at[1, 1], dev_x(3))

    got(yropp.at[0], yo_s.at[0], yo_r.at[0])
    ys[0, 0] = (acc_half(at_y(1), 0) + yropp[0].astype(F32)).astype(BF16)
    send(ys.at[0, 0], yr.at[0, 0], yp_s.at[0, 0], yp_r.at[0, 0], dev_y(1))
    got(yropp.at[1], yo_s.at[1], yo_r.at[1])
    ys[1, 1] = (acc_half(at_y(3), 1) + yropp[1].astype(F32)).astype(BF16)
    send(ys.at[1, 1], yr.at[1, 1], yp_s.at[1, 1], yp_r.at[1, 1], dev_y(3))

    piece = tok // n_z
    for h in (1, 0):
        got(xr.at[0, h], xp_s.at[0, h], xp_r.at[0, h])
        got(xr.at[1, h], xp_s.at[1, h], xp_r.at[1, h])
        total = summed(0, h) + xr[0, h].astype(F32) + xr[1, h].astype(F32)
        at = pl.ds(h * (n_z // 2), n_z // 2)
        Zs[at] = total.reshape(n_z // 2, piece, width).astype(BF16)
    Zr[t] = Zs[t]
    for d in range(1, n_z):
        send(Zs.at[lax.rem(t + d, n_z)], Zr.at[t], z1_s.at[d - 1], z1_r.at[d - 1], dev_z(d))

    total = []
    for h in range(2):
        got(yr.at[0, h], yp_s.at[0, h], yp_r.at[0, h])
        got(yr.at[1, h], yp_s.at[1, h], yp_r.at[1, h])
        value = acc_half(y, h) + yr[0, h].astype(F32) + yr[1, h].astype(F32)
        value = value.astype(BF16)
        for k in range(SIDE):
            R[k, h * cut : (h + 1) * cut, :] = value[:, k * lanes : (k + 1) * lanes]
    OUT[x] = R[x]
    for k, d in enumerate((1, 3, 2)):
        send(R.at[at_x(d)], OUT.at[x], ra_s.at[k], ra_r.at[k], dev_x(d))

    for d in range(1, n_z):
        got(Zr.at[lax.rem(t + n_z - d, n_z)], z1_s.at[d - 1], z1_r.at[d - 1])
    done = Zr[0].astype(F32)
    for k in range(1, n_z):
        done += Zr[k].astype(F32)
    Zf[t] = done.astype(BF16)
    for d in range(1, n_z):
        send(Zf.at[t], Zf.at[t], z2_s.at[d - 1], z2_r.at[d - 1], dev_z(d))

    for k, d in enumerate((1, 3, 2)):
        got(OUT.at[at_x(SIDE - d)], ra_s.at[k], ra_r.at[k])
    for k in range(SIDE):
        at = slice(k * q, (k + 1) * q)
        for i in range(2):
            out_in[i, at, :] = OUT[k, i * q : (i + 1) * q, :].astype(F32)
        out_out[at, :] = OUT[k, 2 * q : 3 * q, :].astype(F32)

    for d in range(1, n_z):
        got(Zf.at[lax.rem(t + n_z - d, n_z)], z2_s.at[d - 1], z2_r.at[d - 1])
    out_tok[...] = Zf[...].astype(F32).reshape(tok, width)
    for copy in pending:
        copy.wait_send()


def shards(n_z, tokens, tangent, cotangent, expert_ids, gates, w_in, v_in, w_out, v_out):
    tok = tokens.shape[0]
    ff, lanes = w_in.shape[2:]
    width = tokens.shape[1]
    q = ff // SIDE
    half = tok // 2
    part = width // SIDE
    cut = 3 * q // 2
    dma = pltpu.SemaphoreType.DMA
    vmem = pl.BlockSpec(memory_space=pltpu.VMEM)
    hbm = pl.BlockSpec(memory_space=pltpu.HBM)
    y_tok, y_in, y_out = pl.pallas_call(
        functools.partial(kernel, n_z),
        out_shape=(
            jax.ShapeDtypeStruct((tok, width), F32),
            jax.ShapeDtypeStruct((2, ff, lanes), F32),
            jax.ShapeDtypeStruct((ff, lanes), F32),
        ),
        in_specs=[vmem, vmem] + [hbm] * 7,
        out_specs=(vmem, vmem, vmem),
        scratch_shapes=[
            pltpu.VMEM((6, q, width), BF16),
            pltpu.VMEM((3, SIDE, 2, tok, width), BF16),
            pltpu.VMEM((2, SIDE, 8, tok), F32),
            pltpu.VMEM((8 * q, 2 * tok), F32),
            pltpu.VMEM((4 * q, 2 * tok), BF16),
            pltpu.VMEM((2 * tok, 4 * q), BF16),
            pltpu.VMEM((q, 2 * tok), BF16),
            pltpu.VMEM((SIDE, 3 * q, part), F32),
            pltpu.VMEM((4, tok, width), F32),
            pltpu.VMEM((4, tok, width), BF16),
            pltpu.VMEM((4, tok, width), BF16),
            pltpu.VMEM((2, 2, half, width), BF16),
            pltpu.VMEM((2, half, width), BF16),
            pltpu.VMEM((2, 2, half, width), BF16),
            pltpu.VMEM((2, half, width), BF16),
            pltpu.VMEM((2, 2, cut, part), BF16),
            pltpu.VMEM((2, cut, part), BF16),
            pltpu.VMEM((2, 2, cut, part), BF16),
            pltpu.VMEM((2, cut, part), BF16),
            pltpu.VMEM((SIDE, 3 * q, lanes), BF16),
            pltpu.VMEM((SIDE, 3 * q, lanes), BF16),
            pltpu.VMEM((n_z, tok // n_z, width), BF16),
            pltpu.VMEM((n_z, tok // n_z, width), BF16),
            pltpu.VMEM((n_z, tok // n_z, width), BF16),
            dma((7,)),
            dma((3, 4)), dma((3, 4)),
            dma((2, 4)), dma((2, 4)),
            dma((2, 4)), dma((2, 4)),
            dma((2, 2)), dma((2, 2)),
            dma((2,)), dma((2,)),
            dma((3,)), dma((3,)),
            dma((2,)),
            dma((4, 2)), dma((4, 2)),
            dma((4,)), dma((4,)),
            dma((2,)), dma((2,)),
            dma((2, 2)), dma((2, 2)),
            dma((2,)), dma((2,)),
            dma((2, 2)), dma((2, 2)),
            dma((3,)), dma((3,)),
            dma((n_z - 1,)), dma((n_z - 1,)),
            dma((n_z - 1,)), dma((n_z - 1,)),
        ],
        compiler_params=pltpu.CompilerParams(
            collective_id=0, has_side_effects=True, vmem_limit_bytes=62 * 1024 * 1024
        ),
    )(
        expert_ids.T, gates.T, tokens, tangent, cotangent, w_in[0], v_in[0], w_out[0], v_out[0]
    )
    return y_tok, y_in[None], y_out[None]


def solution(mesh):
    rows = P(("expert", "dp"), None)
    w_spec = P(("tensor", "expert"), None, None, "dp")
    o_spec = P(("tensor", "expert"), None, "dp")
    return jax.shard_map(
        functools.partial(shards, mesh.shape["tensor"]),
        mesh=mesh,
        in_specs=(rows,) * 5 + (w_spec, w_spec, o_spec, o_spec),
        out_specs=(rows, w_spec, o_spec),
        check_vma=False,
    )
```

```python
import functools

import jax
import jax.numpy as jnp
from jax import lax
from jax.experimental import pallas as pl
from jax.experimental.pallas import tpu as pltpu
from jax.sharding import PartitionSpec as P

MESH = pl.DeviceIdType.MESH
F32 = jnp.float32
BF16 = jnp.bfloat16
SIDE = 4
NT = (((1,), (1,)), ((), ()))
NN = (((1,), (0,)), ((), ()))


def mm(a, b, dims=NN):
    return lax.dot_general(a, b, dims, preferred_element_type=F32)


def kernel(
    n_z, ids_ref, gates_ref, tok_ref, tan_ref, cot_ref, wi_ref, vi_ref, wo_ref, vo_ref,
    out_tok, out_in, out_out,
    W, stage, X, G, C, S, ST, H, acc, Pown, PDs, PDr, xs, xopp, xr, xropp, ys, yopp, yr, yropp, R, OUT, Zs, Zr, Zf,
    loc, wa_s, wa_r, st_s, st_r, sf_s, sf_r, wy_s, wy_r, wf_s, wf_r, xh_s, xh_r, xf_s, xf_r, zx_s, zx_r,
    g_s, g_r, gd, dd_s, dd_r, pd_s, pd_r,
    xo_s, xo_r, xp_s, xp_r, yo_s, yo_r, yp_s, yp_r, ra_s, ra_r, z1_s, z1_r, z2_s, z2_r,
):
    t = lax.axis_index("tensor")
    e = lax.axis_index("expert")
    p = lax.axis_index("dp")
    y, x = p // SIDE, p % SIDE
    color = lax.rem(t, 2)
    tok = tok_ref.shape[0]
    half = tok // 2
    quarter = tok // 4
    lanes = wi_ref.shape[-1]
    q = W.shape[1]
    width = W.shape[2]
    part = width // SIDE

    def at_x(d):
        return lax.rem(x + d, SIDE)

    def at_y(d):
        return lax.rem(y + d, SIDE)

    def dev_x(d):
        return (t, e, y * SIDE + at_x(d))

    def dev_y(d):
        return (t, e, at_y(d) * SIDE + x)

    def dev_z(d):
        return (lax.rem(t + d, n_z), e, p)

    partner = (t, 1 - e, p)
    pending = []

    def send(src, dst, ssem, rsem, dev):
        copy = pltpu.make_async_remote_copy(
            src_ref=src, dst_ref=dst, send_sem=ssem, recv_sem=rsem, device_id=dev, device_id_type=MESH
        )
        copy.start()
        pending.append(copy)

    def got(dst, ssem, rsem):
        pltpu.make_async_remote_copy(
            src_ref=dst, dst_ref=dst, send_sem=ssem, recv_sem=rsem, device_id=partner, device_id_type=MESH
        ).wait_recv()

    barrier = pltpu.get_barrier_semaphore()
    peers = [partner] + [dev_x(d) for d in (1, 2, 3)] + [dev_y(d) for d in (1, 3)] + [dev_z(d) for d in range(1, n_z)]
    for peer in peers:
        pl.semaphore_signal(barrier, inc=1, device_id=peer, device_id_type=MESH)

    def slab(yy, xx):
        return pl.ds(pl.multiple_of((yy * SIDE + xx) * lanes, lanes), lanes)

    def rows(k):
        return pl.ds(pl.multiple_of(k * q, q), q)

    mine = [
        pltpu.make_async_copy(wi_ref.at[:, rows(x), :], W.at[0:2, :, slab(y, x)], loc.at[3]),
        pltpu.make_async_copy(vi_ref.at[:, rows(x), :], W.at[2:4, :, slab(y, x)], loc.at[4]),
        pltpu.make_async_copy(wo_ref.at[rows(x), :], W.at[4, :, slab(y, x)], loc.at[5]),
        pltpu.make_async_copy(vo_ref.at[rows(x), :], W.at[5, :, slab(y, x)], loc.at[6]),
        pltpu.make_async_copy(tok_ref, X.at[0, x, e], loc.at[0]),
        pltpu.make_async_copy(tan_ref, X.at[1, x, e], loc.at[1]),
        pltpu.make_async_copy(cot_ref, X.at[2, x, e], loc.at[2]),
    ]
    for copy in mine:
        copy.start()
    ids, gates = ids_ref[...], gates_ref[...]
    for r in range(2):
        G[e, x, pl.ds(r, 1), :] = jnp.sum(jnp.where(ids == 2 * t + r, gates, 0.0), axis=0, keepdims=True)
    pl.semaphore_wait(barrier, len(peers))

    def thirds(buf, h):
        return (buf.at[h, 0:2], buf.at[h, 2])

    def in_w(h, at):
        return (W.at[2 * h : 2 * h + 2, :, at], W.at[4 + h, :, at])

    def from_args(h, k):
        return ((wi_ref, vi_ref)[h].at[:, rows(k), :], (wo_ref, vo_ref)[h].at[rows(k), :])

    for h in range(2):
        for i, (src, to) in enumerate(zip(from_args(h, at_x(2)), thirds(stage, h))):
            send(src, to, st_s.at[h, i], st_r.at[h, i], dev_x(1 + 2 * h))
    for k, d in enumerate((1, 3)):
        for h in range(2):
            for i, (src, to) in enumerate(zip(from_args(h, at_x(d)), in_w(h, slab(y, x)))):
                send(src, to, wa_s.at[k, 2 * h + i], wa_r.at[k, 2 * h + i], dev_x(d))
    for k, d in enumerate((1, 3, 2)):
        send(G.at[e, x], G.at[e, x], g_s.at[k], g_r.at[k], dev_x(d))
    for copy in mine:
        copy.wait()

    def wslab(yy, d):
        return W.at[:, :, slab(yy, at_x(SIDE - d))]

    def whalf(yy, d, h):
        return W.at[3 * h : 3 * h + 3, :, slab(yy, at_x(SIDE - d))]

    order = (0, 1, 3, 2)

    def spread(d):
        k = order.index(d)
        send(wslab(y, d), wslab(y, d), wy_s.at[0, k], wy_r.at[0, k], dev_y(1))
        send(wslab(y, d), wslab(y, d), wy_s.at[1, k], wy_r.at[1, k], dev_y(3))

    def onward(d):
        k = order.index(d)
        got(wslab(at_y(3), d), wy_s.at[0, k], wy_r.at[0, k])
        send(whalf(at_y(3), d, 0), whalf(at_y(3), d, 0), wf_s.at[0, k], wf_r.at[0, k], dev_y(1))
        got(wslab(at_y(1), d), wy_s.at[1, k], wy_r.at[1, k])
        send(whalf(at_y(1), d, 1), whalf(at_y(1), d, 1), wf_s.at[1, k], wf_r.at[1, k], dev_y(3))

    spread(0)
    send(X.at[:, x, e], X.at[:, x, e], dd_s.at[0, 0, 0], dd_r.at[0, 0, 0], partner)
    for h in range(2):
        for i, to in enumerate(thirds(stage, h)):
            got(to, st_s.at[h, i], st_r.at[h, i])
        for i, (src, to) in enumerate(zip(thirds(stage, h), in_w(h, slab(y, at_x(3 - 2 * h))))):
            send(src, to, sf_s.at[h, i], sf_r.at[h, i], dev_x(1 + 2 * h))

    def piece(a, own, h, core):
        first = (color if own else 1 - color) * half + h * quarter
        return X.at[:, a, core, pl.ds(pl.multiple_of(first, quarter), quarter), :]

    for k, h in ((0, 0), (1, 1), (0, 1), (1, 0)):
        part_of = piece(x, True, h, e)
        send(part_of, part_of, xh_s.at[k, h], xh_r.at[k, h], dev_x(1 + 2 * k))

    def to_core(rel, own, h):
        part_of = piece(at_x(SIDE - rel), own, h, e)
        k = 0 if own else 1
        send(part_of, part_of, dd_s.at[rel, k, h], dd_r.at[rel, k, h], partner)

    def to_planes(rel, h):
        part_of = piece(at_x(SIDE - rel), True, h, e)
        send(part_of, part_of, zx_s.at[rel - 1, h], zx_r.at[rel - 1, h], dev_z(1 if h == 0 else n_z - 1))

    def over_x(rel, h):
        a = at_x(SIDE - rel)
        if rel == 2:
            got(piece(a, True, h, e), xf_s.at[h], xf_r.at[h])
        else:
            k = 0 if rel == 1 else 1
            got(piece(a, True, h, e), xh_s.at[k, h], xh_r.at[k, h])
            if h == k:
                send(piece(a, True, h, e), piece(a, True, h, e), xf_s.at[h], xf_r.at[h], dev_x(1 + 2 * k))
        to_planes(rel, h)
        to_core(rel, True, h)

    def over_z(rel, h):
        got(piece(at_x(SIDE - rel), False, h, e), zx_s.at[rel - 1, h], zx_r.at[rel - 1, h])
        to_core(rel, False, h)

    for k, d in enumerate((1, 3)):
        for h in range(2):
            for i, to in enumerate(in_w(h, slab(y, at_x(SIDE - d)))):
                got(to, wa_s.at[k, 2 * h + i], wa_r.at[k, 2 * h + i])
        spread(d)
    for h in range(2):
        for i, to in enumerate(in_w(h, slab(y, at_x(2)))):
            got(to, sf_s.at[h, i], sf_r.at[h, i])
    spread(2)
    onward(0)
    onward(1)
    over_x(1, 0)
    over_x(3, 1)
    onward(3)
    onward(2)
    for k, d in enumerate((1, 3, 2)):
        got(G.at[e, at_x(SIDE - d)], g_s.at[k], g_r.at[k])
    send(G.at[e], G.at[e], gd.at[0], gd.at[1], partner)
    over_x(1, 1)
    over_x(3, 0)
    over_z(1, 0)
    over_z(3, 1)
    over_x(2, 0)
    over_x(2, 1)
    over_z(3, 0)
    over_z(1, 1)
    for k, d in enumerate(order):
        got(whalf(at_y(2), d, 0), wf_s.at[0, k], wf_r.at[0, k])
        got(whalf(at_y(2), d, 1), wf_s.at[1, k], wf_r.at[1, k])
    got(G.at[1 - e], gd.at[0], gd.at[1])

    n_acc = acc.shape[1]
    cut = n_acc // 2
    step = 32

    def tokens_of(a):
        return pl.ds(pl.multiple_of(a * 2 * tok, 2 * tok), 2 * tok)

    def forward(rel):
        a = at_x(SIDE - rel)
        if rel == 0:
            got(X.at[:, x, 1 - e], dd_s.at[0, 0, 0], dd_r.at[0, 0, 0])
        else:
            for k in range(2):
                for h in range(2):
                    got(piece(a, k == 0, h, 1 - e), dd_s.at[rel, k, h], dd_r.at[rel, k, h])

        def both(i):
            return X[i, a].reshape(2 * tok, width)

        C[0 : 2 * q, :] = mm(W[0:2].reshape(2 * q, width), both(0), NT)
        C[2 * q : 4 * q, :] = mm(W[2:4].reshape(2 * q, width), both(0), NT)
        C[4 * q : 6 * q, :] = mm(W[0:2].reshape(2 * q, width), both(1), NT)
        C[6 * q : 8 * q, :] = mm(W[4:6].reshape(2 * q, width), both(2), NT)
        gate = jnp.concatenate([G[0, a, pl.ds(e, 1), :], G[1, a, pl.ds(e, 1), :]], axis=1)
        cols = tokens_of(a)

        def rows_of(i, carry):
            at = pl.multiple_of(i * step, step)

            def c(k):
                return C[pl.ds(k * q + at, step), :]

            pre, up = c(0), c(1)
            pre_dot, up_dot = c(4) + c(2), c(5) + c(3)
            g, g_dot = c(6) * gate, c(7) * gate
            sigma = jax.nn.sigmoid(pre)
            rest = 1.0 - sigma
            s0 = pre * sigma
            s1 = sigma * (1.0 + pre * rest)
            s2 = sigma * rest * (2.0 + pre * (1.0 - 2.0 * sigma))
            S[pl.ds(at, step), cols] = (
                g_dot * up * s1 + g * up_dot * s1 + g * up * s2 * pre_dot
            ).astype(BF16)
            S[pl.ds(q + at, step), cols] = (g_dot * s0 + g * s1 * pre_dot).astype(BF16)
            S[pl.ds(2 * q + at, step), cols] = (g * up * s1).astype(BF16)
            S[pl.ds(3 * q + at, step), cols] = (g * s0).astype(BF16)
            H[pl.ds(at, step), cols] = ((s1 * pre_dot * up + s0 * up_dot) * gate).astype(BF16)
            return carry

        lax.fori_loop(0, q // step, rows_of, 0)

    def tokens_back(rel):
        ST[...] = S[:, tokens_of(at_x(SIDE - rel))].T

        def columns(n, carry):
            cols = pl.ds(pl.multiple_of(n * part, part), part)
            value = mm(ST[...], W[0:4, :, cols].reshape(4 * q, part))
            for core in range(2):

                @pl.when(e == core)
                def _():
                    Pown[rel, :, cols] = value[core * tok : (core + 1) * tok]
                    PDs[rel, :, cols] = value[(1 - core) * tok : (2 - core) * tok].astype(BF16)

            return carry

        lax.fori_loop(0, SIDE, columns, 0)
        send(PDs.at[rel], PDr.at[rel], pd_s.at[rel], pd_r.at[rel], partner)

    def weights_back(n):
        cols = pl.ds(pl.multiple_of(n * part, part), part)

        def every(i):
            return X[i, :, :, :, cols].reshape(SIDE * 2 * tok, part)

        acc[n, 0 : 2 * q, :] = mm(S[2 * q : 4 * q, :], every(1)) + mm(S[0 : 2 * q, :], every(0))
        acc[n, 2 * q : 3 * q, :] = mm(H[...], every(2))

    def summed(rel, h):
        at = pl.ds(h * half, half)
        return Pown[rel, at, :] + PDr[rel, at, :].astype(F32)

    def acc_half(k, h):
        return acc[k, h * cut : (h + 1) * cut, :]

    forward(0)
    forward(1)
    over_z(2, 0)
    over_z(2, 1)
    forward(3)
    forward(2)

    tokens_back(2)
    tokens_back(1)
    got(PDr.at[2], pd_s.at[2], pd_r.at[2])
    for h in range(2):
        xopp[h] = summed(2, h).astype(BF16)
        send(xopp.at[h], xropp.at[h], xo_s.at[h], xo_r.at[h], dev_x(1 + 2 * h))
    tokens_back(3)
    got(PDr.at[1], pd_s.at[1], pd_r.at[1])
    xs[1, 0] = summed(1, 0).astype(BF16)
    send(xs.at[1, 0], xr.at[1, 0], xp_s.at[1, 0], xp_r.at[1, 0], dev_x(3))
    weights_back(at_y(2))
    for h in range(2):
        yopp[h] = acc_half(at_y(2), h).astype(BF16)
        send(yopp.at[h], yropp.at[h], yo_s.at[h], yo_r.at[h], dev_y(1 + 2 * h))
    got(PDr.at[3], pd_s.at[3], pd_r.at[3])
    xs[0, 1] = summed(3, 1).astype(BF16)
    send(xs.at[0, 1], xr.at[0, 1], xp_s.at[0, 1], xp_r.at[0, 1], dev_x(1))
    weights_back(at_y(1))
    ys[0, 1] = acc_half(at_y(1), 1).astype(BF16)
    send(ys.at[0, 1], yr.at[0, 1], yp_s.at[0, 1], yp_r.at[0, 1], dev_y(1))
    weights_back(at_y(3))
    ys[1, 0] = acc_half(at_y(3), 0).astype(BF16)
    send(ys.at[1, 0], yr.at[1, 0], yp_s.at[1, 0], yp_r.at[1, 0], dev_y(3))
    tokens_back(0)

    got(xropp.at[0], xo_s.at[0], xo_r.at[0])
    xs[0, 0] = (summed(3, 0) + xropp[0].astype(F32)).astype(BF16)
    send(xs.at[0, 0], xr.at[0, 0], xp_s.at[0, 0], xp_r.at[0, 0], dev_x(1))
    got(xropp.at[1], xo_s.at[1], xo_r.at[1])
    xs[1, 1] = (summed(1, 1) + xropp[1].astype(F32)).astype(BF16)
    send(xs.at[1, 1], xr.at[1, 1], xp_s.at[1, 1], xp_r.at[1, 1], dev_x(3))
    weights_back(y)

    got(yropp.at[0], yo_s.at[0], yo_r.at[0])
    ys[0, 0] = (acc_half(at_y(1), 0) + yropp[0].astype(F32)).astype(BF16)
    send(ys.at[0, 0], yr.at[0, 0], yp_s.at[0, 0], yp_r.at[0, 0], dev_y(1))
    got(yropp.at[1], yo_s.at[1], yo_r.at[1])
    ys[1, 1] = (acc_half(at_y(3), 1) + yropp[1].astype(F32)).astype(BF16)
    send(ys.at[1, 1], yr.at[1, 1], yp_s.at[1, 1], yp_r.at[1, 1], dev_y(3))

    piece_z = tok // n_z
    got(PDr.at[0], pd_s.at[0], pd_r.at[0])
    for h in (1, 0):
        got(xr.at[0, h], xp_s.at[0, h], xp_r.at[0, h])
        got(xr.at[1, h], xp_s.at[1, h], xp_r.at[1, h])
        total = summed(0, h) + xr[0, h].astype(F32) + xr[1, h].astype(F32)
        at = pl.ds(h * (n_z // 2), n_z // 2)
        Zs[at] = total.reshape(n_z // 2, piece_z, width).astype(BF16)
    Zr[t] = Zs[t]
    for d in range(1, n_z):
        send(Zs.at[lax.rem(t + d, n_z)], Zr.at[t], z1_s.at[d - 1], z1_r.at[d - 1], dev_z(d))

    for h in range(2):
        got(yr.at[0, h], yp_s.at[0, h], yp_r.at[0, h])
        got(yr.at[1, h], yp_s.at[1, h], yp_r.at[1, h])
        value = acc_half(y, h) + yr[0, h].astype(F32) + yr[1, h].astype(F32)
        value = value.astype(BF16)
        for k in range(SIDE):
            R[k, h * cut : (h + 1) * cut, :] = value[:, k * lanes : (k + 1) * lanes]
    OUT[x] = R[x]
    for k, d in enumerate((1, 3, 2)):
        send(R.at[at_x(d)], OUT.at[x], ra_s.at[k], ra_r.at[k], dev_x(d))

    for d in range(1, n_z):
        got(Zr.at[lax.rem(t + n_z - d, n_z)], z1_s.at[d - 1], z1_r.at[d - 1])
    done = Zr[0].astype(F32)
    for k in range(1, n_z):
        done += Zr[k].astype(F32)
    Zf[t] = done.astype(BF16)
    for d in range(1, n_z):
        send(Zf.at[t], Zf.at[t], z2_s.at[d - 1], z2_r.at[d - 1], dev_z(d))

    for k, d in enumerate((1, 3, 2)):
        got(OUT.at[at_x(SIDE - d)], ra_s.at[k], ra_r.at[k])
    for k in range(SIDE):
        at = slice(k * q, (k + 1) * q)
        for i in range(2):
            out_in[i, at, :] = OUT[k, i * q : (i + 1) * q, :]
        out_out[at, :] = OUT[k, 2 * q : 3 * q, :]

    for d in range(1, n_z):
        got(Zf.at[lax.rem(t + n_z - d, n_z)], z2_s.at[d - 1], z2_r.at[d - 1])
    out_tok[...] = Zf[...].reshape(tok, width)
    for copy in pending:
        copy.wait_send()


def shards(n_z, tokens, tangent, cotangent, expert_ids, gates, w_in, v_in, w_out, v_out):
    tok = tokens.shape[0]
    ff, lanes = w_in.shape[2:]
    width = tokens.shape[1]
    q = ff // SIDE
    half = tok // 2
    part = width // SIDE
    cut = 3 * q // 2
    dma = pltpu.SemaphoreType.DMA
    vmem = pl.BlockSpec(memory_space=pltpu.VMEM)
    hbm = pl.BlockSpec(memory_space=pltpu.HBM)
    y_tok, y_in, y_out = pl.pallas_call(
        functools.partial(kernel, n_z),
        out_shape=(
            jax.ShapeDtypeStruct((tok, width), BF16),
            jax.ShapeDtypeStruct((2, ff, lanes), BF16),
            jax.ShapeDtypeStruct((ff, lanes), BF16),
        ),
        in_specs=[vmem, vmem] + [hbm] * 7,
        out_specs=(vmem, vmem, vmem),
        scratch_shapes=[
            pltpu.VMEM((6, q, width), BF16),
            pltpu.VMEM((2, 3, q, lanes), BF16),
            pltpu.VMEM((3, SIDE, 2, tok, width), BF16),
            pltpu.VMEM((2, SIDE, 8, tok), F32),
            pltpu.VMEM((8 * q, 2 * tok), F32),
            pltpu.VMEM((4 * q, SIDE * 2 * tok), BF16),
            pltpu.VMEM((2 * tok, 4 * q), BF16),
            pltpu.VMEM((q, SIDE * 2 * tok), BF16),
            pltpu.VMEM((SIDE, 3 * q, part), F32),
            pltpu.VMEM((4, tok, width), F32),
            pltpu.VMEM((4, tok, width), BF16),
            pltpu.VMEM((4, tok, width), BF16),
            pltpu.VMEM((2, 2, half, width), BF16),
            pltpu.VMEM((2, half, width), BF16),
            pltpu.VMEM((2, 2, half, width), BF16),
            pltpu.VMEM((2, half, width), BF16),
            pltpu.VMEM((2, 2, cut, part), BF16),
            pltpu.VMEM((2, cut, part), BF16),
            pltpu.VMEM((2, 2, cut, part), BF16),
            pltpu.VMEM((2, cut, part), BF16),
            pltpu.VMEM((SIDE, 3 * q, lanes), BF16),
            pltpu.VMEM((SIDE, 3 * q, lanes), BF16),
            pltpu.VMEM((n_z, tok // n_z, width), BF16),
            pltpu.VMEM((n_z, tok // n_z, width), BF16),
            pltpu.VMEM((n_z, tok // n_z, width), BF16),
            dma((7,)),
            dma((2, 4)), dma((2, 4)),
            dma((2, 2)), dma((2, 2)),
            dma((2, 2)), dma((2, 2)),
            dma((2, 4)), dma((2, 4)),
            dma((2, 4)), dma((2, 4)),
            dma((2, 2)), dma((2, 2)),
            dma((2,)), dma((2,)),
            dma((3, 2)), dma((3, 2)),
            dma((3,)), dma((3,)),
            dma((2,)),
            dma((4, 2, 2)), dma((4, 2, 2)),
            dma((4,)), dma((4,)),
            dma((2,)), dma((2,)),
            dma((2, 2)), dma((2, 2)),
            dma((2,)), dma((2,)),
            dma((2, 2)), dma((2, 2)),
            dma((3,)), dma((3,)),
            dma((n_z - 1,)), dma((n_z - 1,)),
            dma((n_z - 1,)), dma((n_z - 1,)),
        ],
        compiler_params=pltpu.CompilerParams(
            collective_id=0, has_side_effects=True, vmem_limit_bytes=62 * 1024 * 1024
        ),
    )(
        expert_ids.T, gates.T, tokens, tangent, cotangent, w_in[0], v_in[0], w_out[0], v_out[0]
    )
    return y_tok.astype(F32), y_in[None].astype(F32), y_out[None].astype(F32)


def solution(mesh):
    rows = P(("expert", "dp"), None)
    w_spec = P(("tensor", "expert"), None, None, "dp")
    o_spec = P(("tensor", "expert"), None, "dp")
    return jax.shard_map(
        functools.partial(shards, mesh.shape["tensor"]),
        mesh=mesh,
        in_specs=(rows,) * 5 + (w_spec, w_spec, o_spec, o_spec),
        out_specs=(rows, w_spec, o_spec),
        check_vma=False,
    )
```

```python
import functools

import jax
import jax.numpy as jnp
from jax import lax
from jax.experimental import pallas as pl
from jax.experimental.pallas import tpu as pltpu
from jax.sharding import PartitionSpec as P

MESH = pl.DeviceIdType.MESH
F32 = jnp.float32
BF16 = jnp.bfloat16
SIDE = 4
NT = (((1,), (1,)), ((), ()))
NN = (((1,), (0,)), ((), ()))


def mm(a, b, dims=NN):
    return lax.dot_general(a, b, dims, preferred_element_type=F32)


def kernel(
    n_z, ids_ref, gates_ref, tok_ref, tan_ref, cot_ref, wi_ref, vi_ref, wo_ref, vo_ref,
    out_tok, out_in, out_out,
    W, stage, X, G, C, S, ST, H, acc, Pown, PDs, PDr, xs, xopp, xr, xropp, ys, yopp, yr, yropp, R, OUT, Zs, Zr, Zf,
    loc, wa_s, wa_r, st_s, st_r, sf_s, sf_r, wy_s, wy_r, wf_s, wf_r, xh_s, xh_r, xf_s, xf_r, zx_s, zx_r, zo_s, zo_r,
    g_s, g_r, gd, dd_s, dd_r, pd_s, pd_r,
    xo_s, xo_r, xp_s, xp_r, yo_s, yo_r, yp_s, yp_r, ra_s, ra_r, z1_s, z1_r, z2_s, z2_r,
):
    t = lax.axis_index("tensor")
    e = lax.axis_index("expert")
    p = lax.axis_index("dp")
    y, x = p // SIDE, p % SIDE
    color = lax.rem(t, 2)
    tok = tok_ref.shape[0]
    half = tok // 2
    quarter = tok // 4
    lanes = wi_ref.shape[-1]
    q = W.shape[1]
    width = W.shape[2]
    part = width // SIDE

    def at_x(d):
        return lax.rem(x + d, SIDE)

    def at_y(d):
        return lax.rem(y + d, SIDE)

    def dev_x(d):
        return (t, e, y * SIDE + at_x(d))

    def dev_y(d):
        return (t, e, at_y(d) * SIDE + x)

    def dev_z(d):
        return (lax.rem(t + d, n_z), e, p)

    partner = (t, 1 - e, p)
    pending = []

    def send(src, dst, ssem, rsem, dev):
        copy = pltpu.make_async_remote_copy(
            src_ref=src, dst_ref=dst, send_sem=ssem, recv_sem=rsem, device_id=dev, device_id_type=MESH
        )
        copy.start()
        pending.append(copy)

    def got(dst, ssem, rsem):
        pltpu.make_async_remote_copy(
            src_ref=dst, dst_ref=dst, send_sem=ssem, recv_sem=rsem, device_id=partner, device_id_type=MESH
        ).wait_recv()

    barrier = pltpu.get_barrier_semaphore()
    peers = [partner] + [dev_x(d) for d in (1, 2, 3)] + [dev_y(d) for d in (1, 3)] + [dev_z(d) for d in range(1, n_z)]
    for peer in peers:
        pl.semaphore_signal(barrier, inc=1, device_id=peer, device_id_type=MESH)

    def slab(yy, xx):
        return pl.ds(pl.multiple_of((yy * SIDE + xx) * lanes, lanes), lanes)

    def rows(k):
        return pl.ds(pl.multiple_of(k * q, q), q)

    mine = [
        pltpu.make_async_copy(wi_ref.at[:, rows(x), :], W.at[0:2, :, slab(y, x)], loc.at[3]),
        pltpu.make_async_copy(wo_ref.at[rows(x), :], W.at[2, :, slab(y, x)], loc.at[4]),
        pltpu.make_async_copy(vi_ref.at[:, rows(x), :], W.at[3:5, :, slab(y, x)], loc.at[5]),
        pltpu.make_async_copy(vo_ref.at[rows(x), :], W.at[5, :, slab(y, x)], loc.at[6]),
        pltpu.make_async_copy(tok_ref, X.at[0, x, e], loc.at[0]),
        pltpu.make_async_copy(tan_ref, X.at[1, x, e], loc.at[1]),
        pltpu.make_async_copy(cot_ref, X.at[2, x, e], loc.at[2]),
    ]
    for copy in mine:
        copy.start()
    ids, gates = ids_ref[...], gates_ref[...]
    for r in range(2):
        G[e, x, pl.ds(r, 1), :] = jnp.sum(jnp.where(ids == 2 * t + r, gates, 0.0), axis=0, keepdims=True)
    pl.semaphore_wait(barrier, len(peers))

    def thirds(buf, h):
        return (buf.at[h, 0:2], buf.at[h, 2])

    def in_w(h, at):
        return (W.at[3 * h : 3 * h + 2, :, at], W.at[3 * h + 2, :, at])

    def from_args(h, k):
        return ((wi_ref, vi_ref)[h].at[:, rows(k), :], (wo_ref, vo_ref)[h].at[rows(k), :])

    def quarter_to(h):
        for k, d in enumerate((1, 3)):
            for i, (src, to) in enumerate(zip(from_args(h, at_x(d)), in_w(h, slab(y, x)))):
                send(src, to, wa_s.at[k, 2 * h + i], wa_r.at[k, 2 * h + i], dev_x(d))

    quarter_to(0)
    for h in range(2):
        for i, (src, to) in enumerate(zip(from_args(h, at_x(2)), thirds(stage, h))):
            send(src, to, st_s.at[h, i], st_r.at[h, i], dev_x(1 + 2 * h))
    quarter_to(1)
    for k, d in enumerate((1, 3, 2)):
        send(G.at[e, x], G.at[e, x], g_s.at[k], g_r.at[k], dev_x(d))
    for copy in mine:
        copy.wait()

    def unit(yy, d, h):
        return W.at[3 * h : 3 * h + 3, :, slab(yy, at_x(SIDE - d))]

    order = (0, 1, 3, 2)

    def spread(d, h):
        k = order.index(d)
        for i in range(2):
            send(unit(y, d, h), unit(y, d, h), wy_s.at[i, k, h], wy_r.at[i, k, h], dev_y(1 + 2 * i))

    def onward(d):
        k = order.index(d)
        for h in range(2):
            at = unit(at_y(3 - 2 * h), d, h)
            got(at, wy_s.at[h, k, h], wy_r.at[h, k, h])
            send(at, at, wf_s.at[h, k], wf_r.at[h, k], dev_y(1 + 2 * h))

    def got_quarter(h):
        for k, d in enumerate((1, 3)):
            for i, to in enumerate(in_w(h, slab(y, at_x(SIDE - d)))):
                got(to, wa_s.at[k, 2 * h + i], wa_r.at[k, 2 * h + i])
            spread(d, h)

    spread(0, 0)
    spread(0, 1)
    send(X.at[:, x, e], X.at[:, x, e], dd_s.at[0, 0, 0], dd_r.at[0, 0, 0], partner)
    got_quarter(0)
    for h in range(2):
        for i, to in enumerate(thirds(stage, h)):
            got(to, st_s.at[h, i], st_r.at[h, i])
        for i, (src, to) in enumerate(zip(thirds(stage, h), in_w(h, slab(y, at_x(3 - 2 * h))))):
            send(src, to, sf_s.at[h, i], sf_r.at[h, i], dev_x(1 + 2 * h))

    def piece(a, own, h, core):
        first = (color if own else 1 - color) * half + h * quarter
        return X.at[:, a, core, pl.ds(pl.multiple_of(first, quarter), quarter), :]

    for k, h in ((0, 0), (1, 1), (0, 1), (1, 0)):
        part_of = piece(x, True, h, e)
        send(part_of, part_of, xh_s.at[k, h], xh_r.at[k, h], dev_x(1 + 2 * k))

    def to_core(rel, own, h):
        part_of = piece(at_x(SIDE - rel), own, h, e)
        k = 0 if own else 1
        send(part_of, part_of, dd_s.at[rel, k, h], dd_r.at[rel, k, h], partner)

    def eighth(a, own, h, s, core):
        first = (color if own else 1 - color) * half + h * quarter + s * (quarter // 2)
        return X.at[:, a, core, pl.ds(pl.multiple_of(first, quarter // 2), quarter // 2), :]

    def over_x(rel, h):
        a = at_x(SIDE - rel)
        plane = dev_z(1 if h == 0 else n_z - 1)
        if rel == 2:
            for s in range(2):
                at = eighth(a, True, h, s, e)
                got(at, xf_s.at[h, s], xf_r.at[h, s])
                send(at, at, zo_s.at[h, s], zo_r.at[h, s], plane)
        else:
            k = 0 if rel == 1 else 1
            at = piece(a, True, h, e)
            got(at, xh_s.at[k, h], xh_r.at[k, h])
            if h == k:
                for s in range(2):
                    sub = eighth(a, True, h, s, e)
                    send(sub, sub, xf_s.at[h, s], xf_r.at[h, s], dev_x(1 + 2 * k))
            send(at, at, zx_s.at[rel // 2, h], zx_r.at[rel // 2, h], plane)
        to_core(rel, True, h)

    def over_z(rel, h):
        a = at_x(SIDE - rel)
        if rel == 2:
            for s in range(2):
                got(eighth(a, False, h, s, e), zo_s.at[h, s], zo_r.at[h, s])
        else:
            got(piece(a, False, h, e), zx_s.at[rel // 2, h], zx_r.at[rel // 2, h])
        to_core(rel, False, h)

    got_quarter(1)
    for h in range(2):
        for i, to in enumerate(in_w(h, slab(y, at_x(2)))):
            got(to, sf_s.at[h, i], sf_r.at[h, i])
        spread(2, h)
    onward(0)
    onward(1)
    onward(3)
    over_x(1, 0)
    over_x(3, 1)
    onward(2)
    for k, d in enumerate((1, 3, 2)):
        got(G.at[e, at_x(SIDE - d)], g_s.at[k], g_r.at[k])
    send(G.at[e], G.at[e], gd.at[0], gd.at[1], partner)
    over_x(1, 1)
    over_x(3, 0)
    over_z(1, 0)
    over_z(3, 1)
    over_x(2, 0)
    over_x(2, 1)
    over_z(3, 0)
    over_z(1, 1)
    for k, d in enumerate(order):
        for h in range(2):
            got(unit(at_y(3 - 2 * h), d, 1 - h), wy_s.at[h, k, 1 - h], wy_r.at[h, k, 1 - h])
            got(unit(at_y(2), d, h), wf_s.at[h, k], wf_r.at[h, k])
    got(G.at[1 - e], gd.at[0], gd.at[1])

    n_acc = acc.shape[1]
    cut = n_acc // 2
    step = 32

    def tokens_of(a):
        return pl.ds(pl.multiple_of(a * 2 * tok, 2 * tok), 2 * tok)

    def forward(rel):
        a = at_x(SIDE - rel)
        if rel == 0:
            got(X.at[:, x, 1 - e], dd_s.at[0, 0, 0], dd_r.at[0, 0, 0])
        else:
            for k in range(2):
                for h in range(2):
                    got(piece(a, k == 0, h, 1 - e), dd_s.at[rel, k, h], dd_r.at[rel, k, h])

        def both(i):
            return X[i, a].reshape(2 * tok, width)

        C[0 : 2 * q, :] = mm(W[0:2].reshape(2 * q, width), both(0), NT)
        C[2 * q : 4 * q, :] = mm(W[3:5].reshape(2 * q, width), both(0), NT)
        C[4 * q : 6 * q, :] = mm(W[0:2].reshape(2 * q, width), both(1), NT)
        C[6 * q : 7 * q, :] = mm(W[2], both(2), NT)
        C[7 * q : 8 * q, :] = mm(W[5], both(2), NT)
        gate = jnp.concatenate([G[0, a, pl.ds(e, 1), :], G[1, a, pl.ds(e, 1), :]], axis=1)
        cols = tokens_of(a)

        def rows_of(i, carry):
            at = pl.multiple_of(i * step, step)

            def c(k):
                return C[pl.ds(k * q + at, step), :]

            pre, up = c(0), c(1)
            pre_dot, up_dot = c(4) + c(2), c(5) + c(3)
            g, g_dot = c(6) * gate, c(7) * gate
            sigma = jax.nn.sigmoid(pre)
            rest = 1.0 - sigma
            s0 = pre * sigma
            s1 = sigma * (1.0 + pre * rest)
            s2 = sigma * rest * (2.0 + pre * (1.0 - 2.0 * sigma))
            S[pl.ds(at, step), cols] = (
                g_dot * up * s1 + g * up_dot * s1 + g * up * s2 * pre_dot
            ).astype(BF16)
            S[pl.ds(q + at, step), cols] = (g_dot * s0 + g * s1 * pre_dot).astype(BF16)
            S[pl.ds(2 * q + at, step), cols] = (g * up * s1).astype(BF16)
            S[pl.ds(3 * q + at, step), cols] = (g * s0).astype(BF16)
            H[pl.ds(at, step), cols] = ((s1 * pre_dot * up + s0 * up_dot) * gate).astype(BF16)
            return carry

        lax.fori_loop(0, q // step, rows_of, 0)
        ST[rel] = S[:, cols].T

    def tokens_back(n):
        cols = slice(n * part, (n + 1) * part)
        for rel in (2, 1, 3, 0):
            value = mm(ST[rel, :, 0 : 2 * q], W[0:2, :, cols].reshape(2 * q, part))
            value += mm(ST[rel, :, 2 * q : 4 * q], W[3:5, :, cols].reshape(2 * q, part))
            for core in range(2):

                @pl.when(e == core)
                def _():
                    Pown[rel, n] = value[core * tok : (core + 1) * tok]
                    PDs[rel, n] = value[(1 - core) * tok : (2 - core) * tok].astype(BF16)

            send(PDs.at[rel, n], PDr.at[rel, n], pd_s.at[rel, n], pd_r.at[rel, n], partner)

    def weights_back(n):
        cols = pl.ds(pl.multiple_of(n * part, part), part)

        def every(i):
            return X[i, :, :, :, cols].reshape(SIDE * 2 * tok, part)

        acc[n, 0 : 2 * q, :] = mm(S[2 * q : 4 * q, :], every(1)) + mm(S[0 : 2 * q, :], every(0))
        acc[n, 2 * q : 3 * q, :] = mm(H[...], every(2))

    def summed(rel, n, h):
        at = pl.ds(h * half, half)
        return Pown[rel, n, at, :] + PDr[rel, n, at, :].astype(F32)

    def acc_half(k, h):
        return acc[k, h * cut : (h + 1) * cut, :]

    def x_first(n):
        for rel in (2, 1, 3):
            got(PDr.at[rel, n], pd_s.at[rel, n], pd_r.at[rel, n])
            if rel == 2:
                for h in range(2):
                    xopp[n, h] = summed(2, n, h).astype(BF16)
                    send(xopp.at[n, h], xropp.at[n, h], xo_s.at[n, h], xo_r.at[n, h], dev_x(1 + 2 * h))
            else:
                k, h = (1, 0) if rel == 1 else (0, 1)
                xs[n, k, h] = summed(rel, n, h).astype(BF16)
                send(xs.at[n, k, h], xr.at[n, k, h], xp_s.at[n, k, h], xp_r.at[n, k, h], dev_x(1 + 2 * k))

    def x_second(n):
        for k in range(2):
            got(xropp.at[n, k], xo_s.at[n, k], xo_r.at[n, k])
            xs[n, k, k] = (summed(3 - 2 * k, n, k) + xropp[n, k].astype(F32)).astype(BF16)
            send(xs.at[n, k, k], xr.at[n, k, k], xp_s.at[n, k, k], xp_r.at[n, k, k], dev_x(1 + 2 * k))

    piece_z = tok // n_z

    def z_scatter(n):
        got(PDr.at[0, n], pd_s.at[0, n], pd_r.at[0, n])
        for h in range(2):
            for k in range(2):
                got(xr.at[n, k, h], xp_s.at[n, k, h], xp_r.at[n, k, h])
            total = summed(0, n, h) + xr[n, 0, h].astype(F32) + xr[n, 1, h].astype(F32)
            at = pl.ds(h * (n_z // 2), n_z // 2)
            Zs[n, at] = total.reshape(n_z // 2, piece_z, part).astype(BF16)
        Zr[n, t] = Zs[n, t]
        for d in range(1, n_z):
            send(Zs.at[n, lax.rem(t + d, n_z)], Zr.at[n, t], z1_s.at[n, d - 1], z1_r.at[n, d - 1], dev_z(d))

    def z_gather(n):
        for d in range(1, n_z):
            got(Zr.at[n, lax.rem(t + n_z - d, n_z)], z1_s.at[n, d - 1], z1_r.at[n, d - 1])
        done = Zr[n, 0].astype(F32)
        for k in range(1, n_z):
            done += Zr[n, k].astype(F32)
        Zf[n, t] = done.astype(BF16)
        for d in range(1, n_z):
            send(Zf.at[n, t], Zf.at[n, t], z2_s.at[n, d - 1], z2_r.at[n, d - 1], dev_z(d))

    def y_first():
        weights_back(at_y(2))
        for h in range(2):
            yopp[h] = acc_half(at_y(2), h).astype(BF16)
            send(yopp.at[h], yropp.at[h], yo_s.at[h], yo_r.at[h], dev_y(1 + 2 * h))

    def y_next(k):
        h = 1 - k
        weights_back(at_y(1 + 2 * k))
        ys[k, h] = acc_half(at_y(1 + 2 * k), h).astype(BF16)
        send(ys.at[k, h], yr.at[k, h], yp_s.at[k, h], yp_r.at[k, h], dev_y(1 + 2 * k))

    def y_second():
        for k in range(2):
            got(yropp.at[k], yo_s.at[k], yo_r.at[k])
            ys[k, k] = (acc_half(at_y(1 + 2 * k), k) + yropp[k].astype(F32)).astype(BF16)
            send(ys.at[k, k], yr.at[k, k], yp_s.at[k, k], yp_r.at[k, k], dev_y(1 + 2 * k))

    def x_slices():
        for h in range(2):
            for k in range(2):
                got(yr.at[k, h], yp_s.at[k, h], yp_r.at[k, h])
            value = acc_half(y, h) + yr[0, h].astype(F32) + yr[1, h].astype(F32)
            value = value.astype(BF16)
            for k in range(SIDE):
                R[h, k] = value[:, k * lanes : (k + 1) * lanes]
            OUT[x, h] = R[h, x]
            for k, d in enumerate((1, 3, 2)):
                send(R.at[h, at_x(d)], OUT.at[x, h], ra_s.at[h, k], ra_r.at[h, k], dev_x(d))

    forward(0)
    forward(1)
    over_z(2, 0)
    over_z(2, 1)
    forward(3)
    forward(2)
    tokens_back(0)
    x_first(0)
    y_first()
    tokens_back(1)
    x_first(1)
    x_second(0)
    tokens_back(2)
    x_first(2)
    y_next(0)
    x_second(1)
    tokens_back(3)
    x_first(3)
    y_next(1)
    x_second(2)
    z_scatter(0)
    weights_back(y)
    x_second(3)
    z_scatter(1)
    y_second()
    z_scatter(2)
    z_gather(0)
    z_scatter(3)
    z_gather(1)
    x_slices()
    z_gather(2)
    z_gather(3)

    for h in range(2):
        for k, d in enumerate((1, 3, 2)):
            got(OUT.at[at_x(SIDE - d), h], ra_s.at[h, k], ra_r.at[h, k])
    for k in range(SIDE):
        at = slice(k * q, (k + 1) * q)
        whole = OUT[k].reshape(n_acc, lanes)
        for i in range(2):
            out_in[i, at, :] = whole[i * q : (i + 1) * q]
        out_out[at, :] = whole[2 * q : 3 * q]

    for n in range(SIDE):
        for d in range(1, n_z):
            got(Zf.at[n, lax.rem(t + n_z - d, n_z)], z2_s.at[n, d - 1], z2_r.at[n, d - 1])
        out_tok[:, n * part : (n + 1) * part] = Zf[n].reshape(tok, part)
    for copy in pending:
        copy.wait_send()


def shards(n_z, tokens, tangent, cotangent, expert_ids, gates, w_in, v_in, w_out, v_out):
    tok = tokens.shape[0]
    ff, lanes = w_in.shape[2:]
    width = tokens.shape[1]
    q = ff // SIDE
    half = tok // 2
    part = width // SIDE
    cut = 3 * q // 2
    dma = pltpu.SemaphoreType.DMA
    vmem = pl.BlockSpec(memory_space=pltpu.VMEM)
    hbm = pl.BlockSpec(memory_space=pltpu.HBM)
    y_tok, y_in, y_out = pl.pallas_call(
        functools.partial(kernel, n_z),
        out_shape=(
            jax.ShapeDtypeStruct((tok, width), BF16),
            jax.ShapeDtypeStruct((2, ff, lanes), BF16),
            jax.ShapeDtypeStruct((ff, lanes), BF16),
        ),
        in_specs=[vmem, vmem] + [hbm] * 7,
        out_specs=(vmem, vmem, vmem),
        scratch_shapes=[
            pltpu.VMEM((6, q, width), BF16),
            pltpu.VMEM((2, 3, q, lanes), BF16),
            pltpu.VMEM((3, SIDE, 2, tok, width), BF16),
            pltpu.VMEM((2, SIDE, 8, tok), F32),
            pltpu.VMEM((8 * q, 2 * tok), F32),
            pltpu.VMEM((4 * q, SIDE * 2 * tok), BF16),
            pltpu.VMEM((4, 2 * tok, 4 * q), BF16),
            pltpu.VMEM((q, SIDE * 2 * tok), BF16),
            pltpu.VMEM((SIDE, 3 * q, part), F32),
            pltpu.VMEM((4, SIDE, tok, part), F32),
            pltpu.VMEM((4, SIDE, tok, part), BF16),
            pltpu.VMEM((4, SIDE, tok, part), BF16),
            pltpu.VMEM((SIDE, 2, 2, half, part), BF16),
            pltpu.VMEM((SIDE, 2, half, part), BF16),
            pltpu.VMEM((SIDE, 2, 2, half, part), BF16),
            pltpu.VMEM((SIDE, 2, half, part), BF16),
            pltpu.VMEM((2, 2, cut, part), BF16),
            pltpu.VMEM((2, cut, part), BF16),
            pltpu.VMEM((2, 2, cut, part), BF16),
            pltpu.VMEM((2, cut, part), BF16),
            pltpu.VMEM((2, SIDE, cut, lanes), BF16),
            pltpu.VMEM((SIDE, 2, cut, lanes), BF16),
            pltpu.VMEM((SIDE, n_z, tok // n_z, part), BF16),
            pltpu.VMEM((SIDE, n_z, tok // n_z, part), BF16),
            pltpu.VMEM((SIDE, n_z, tok // n_z, part), BF16),
            dma((7,)),
            dma((2, 4)), dma((2, 4)),
            dma((2, 2)), dma((2, 2)),
            dma((2, 2)), dma((2, 2)),
            dma((2, 4, 2)), dma((2, 4, 2)),
            dma((2, 4)), dma((2, 4)),
            dma((2, 2)), dma((2, 2)),
            dma((2, 2)), dma((2, 2)),
            dma((2, 2)), dma((2, 2)),
            dma((2, 2)), dma((2, 2)),
            dma((3,)), dma((3,)),
            dma((2,)),
            dma((4, 2, 2)), dma((4, 2, 2)),
            dma((4, 4)), dma((4, 4)),
            dma((4, 2)), dma((4, 2)),
            dma((4, 2, 2)), dma((4, 2, 2)),
            dma((2,)), dma((2,)),
            dma((2, 2)), dma((2, 2)),
            dma((2, 3)), dma((2, 3)),
            dma((4, n_z - 1)), dma((4, n_z - 1)),
            dma((4, n_z - 1)), dma((4, n_z - 1)),
        ],
        compiler_params=pltpu.CompilerParams(
            collective_id=0, has_side_effects=True, vmem_limit_bytes=62 * 1024 * 1024
        ),
    )(
        expert_ids.T, gates.T, tokens, tangent, cotangent, w_in[0], v_in[0], w_out[0], v_out[0]
    )
    return y_tok.astype(F32), y_in[None].astype(F32), y_out[None].astype(F32)


def solution(mesh):
    rows = P(("expert", "dp"), None)
    w_spec = P(("tensor", "expert"), None, None, "dp")
    o_spec = P(("tensor", "expert"), None, "dp")
    return jax.shard_map(
        functools.partial(shards, mesh.shape["tensor"]),
        mesh=mesh,
        in_specs=(rows,) * 5 + (w_spec, w_spec, o_spec, o_spec),
        out_specs=(rows, w_spec, o_spec),
        check_vma=False,
    )
```

```python
import functools

import jax
import jax.numpy as jnp
from jax import lax
from jax.experimental import pallas as pl
from jax.experimental.pallas import tpu as pltpu
from jax.sharding import PartitionSpec as P

MESH = pl.DeviceIdType.MESH
F32 = jnp.float32
BF16 = jnp.bfloat16
SIDE = 4
NT = (((1,), (1,)), ((), ()))
NN = (((1,), (0,)), ((), ()))


def mm(a, b, dims=NN):
    return lax.dot_general(a, b, dims, preferred_element_type=F32)


def kernel(
    n_z, ids_ref, gates_ref, tok_ref, tan_ref, cot_ref, wi_ref, vi_ref, wo_ref, vo_ref,
    out_tok, out_in, out_out,
    W, Wsrc, stage, X, G, C, S, ST, H, acc, Pown, PDs, PDr, xs, xopp, xr, xropp, ys, yopp, yr, yropp, R, OUT, Zt, Zs, Z3, Zm, Zr, Zf,
    loc, snd, wa_r, st_r, sf_r, wy_r, wrest, xh_r, xf_r, zx_r, g_r, dd_r, pd_r, xo_r, xp_r, yo_r, yp_r, ra_r,
    z1_r, z4_r, z2_r, zd_r,
):
    t = lax.axis_index("tensor")
    e = lax.axis_index("expert")
    p = lax.axis_index("dp")
    y, x = p // SIDE, p % SIDE
    color = lax.rem(t, 2)
    tok = tok_ref.shape[0]
    half = tok // 2
    quarter = tok // 4
    lanes = wi_ref.shape[-1]
    q = W.shape[2]
    width = tok_ref.shape[1]
    part = width // SIDE

    def at_x(d):
        return lax.rem(x + d, SIDE)

    def at_y(d):
        return lax.rem(y + d, SIDE)

    def dev_x(d):
        return (t, e, y * SIDE + at_x(d))

    def dev_y(d):
        return (t, e, at_y(d) * SIDE + x)

    def dev_z(d):
        return (lax.rem(t + d, n_z), e, p)

    partner = (t, 1 - e, p)
    s_w, s_x, s_pd, s_xo, s_xs, s_yo, s_ys, s_r, s_z, s_g, s_gd = (snd.at[i] for i in range(11))

    def send(src, dst, ssem, rsem, dev):
        pltpu.make_async_remote_copy(
            src_ref=src, dst_ref=dst, send_sem=ssem, recv_sem=rsem, device_id=dev, device_id_type=MESH
        ).start()

    def got(ref, rsem):
        pltpu.make_async_remote_copy(
            src_ref=ref, dst_ref=ref, send_sem=s_w, recv_sem=rsem, device_id=partner, device_id_type=MESH
        ).wait_recv()

    def sent(ref, ssem):
        pltpu.make_async_remote_copy(
            src_ref=ref, dst_ref=ref, send_sem=ssem, recv_sem=ssem, device_id=partner, device_id_type=MESH
        ).wait_send()

    barrier = pltpu.get_barrier_semaphore()
    peers = [partner] + [dev_x(d) for d in (1, 2, 3)] + [dev_y(d) for d in (1, 3)] + [dev_z(d) for d in (1, 2, n_z - 2, n_z - 1)]
    for peer in peers:
        pl.semaphore_signal(barrier, inc=1, device_id=peer, device_id_type=MESH)

    def rows(k):
        return pl.ds(pl.multiple_of(k * q, q), q)

    for src, dst, i in (
        (wi_ref, Wsrc.at[0:2], 0),
        (wo_ref, Wsrc.at[2], 0),
        (vi_ref, Wsrc.at[3:5], 0),
        (vo_ref, Wsrc.at[5], 0),
        (wi_ref.at[:, rows(x), :], W.at[p, 0:2], 1),
        (wo_ref.at[rows(x), :], W.at[p, 2], 1),
        (vi_ref.at[:, rows(x), :], W.at[p, 3:5], 1),
        (vo_ref.at[rows(x), :], W.at[p, 5], 1),
        (tok_ref, X.at[0, x, e], 2),
        (tan_ref, X.at[1, x, e], 2),
        (cot_ref, X.at[2, x, e], 2),
    ):
        pltpu.make_async_copy(src, dst, loc.at[i]).start()
    ids, gates = ids_ref[...], gates_ref[...]
    for r in range(2):
        G[e, x, pl.ds(r, 1), :] = jnp.sum(jnp.where(ids == 2 * t + r, gates, 0.0), axis=0, keepdims=True)
    pl.semaphore_wait(barrier, len(peers))

    got(Wsrc, loc.at[0])

    def quarter_of(h, k):
        return Wsrc.at[3 * h : 3 * h + 3, rows(k), :]

    def unit(yy, d, h):
        return W.at[yy * SIDE + at_x(SIDE - d), 3 * h : 3 * h + 3]

    def quarter_to(h):
        for k, d in enumerate((1, 3)):
            send(quarter_of(h, at_x(d)), unit(y, 0, h), s_w, wa_r.at[k, h], dev_x(d))

    quarter_to(0)
    for h in range(2):
        send(quarter_of(h, at_x(2)), stage.at[h], s_w, st_r.at[h], dev_x(1 + 2 * h))
    quarter_to(1)
    for d in (1, 3, 2):
        send(G.at[e, x], G.at[e, x], s_g, g_r.at[0], dev_x(d))
    got(W.at[p], loc.at[1])

    order = (0, 1, 3, 2)

    def spread(d, h):
        k = order.index(d)
        for i in range(2):
            sem = wy_r.at[i, k] if i == h else wrest.at[0]
            send(unit(y, d, h), unit(y, d, h), s_w, sem, dev_y(1 + 2 * i))

    def onward(d):
        k = order.index(d)
        for h in range(2):
            at = unit(at_y(3 - 2 * h), d, h)
            got(at, wy_r.at[h, k])
            send(at, at, s_w, wrest.at[0], dev_y(1 + 2 * h))

    def got_quarter(h):
        for k, d in enumerate((1, 3)):
            got(unit(y, d, h), wa_r.at[k, h])
            spread(d, h)

    spread(0, 0)
    spread(0, 1)
    got(X.at[:, x, e], loc.at[2])
    send(X.at[:, x, e], X.at[:, x, e], s_x, dd_r.at[0], partner)
    got_quarter(0)
    for h in range(2):
        got(stage.at[h], st_r.at[h])
        send(stage.at[h], unit(y, 1 + 2 * h, h), s_w, sf_r.at[h], dev_x(1 + 2 * h))

    def piece(a, own, h, i):
        eighth = quarter // 2
        first = (color if own else 1 - color) * half + h * quarter + i * eighth
        return X.at[:, a, e, pl.ds(pl.multiple_of(first, eighth), eighth), :]

    for k, h in ((0, 0), (1, 1), (0, 1), (1, 0)):
        for i in range(2):
            at = piece(x, True, h, i)
            send(at, at, s_x, xh_r.at[k, h, i], dev_x(1 + 2 * k))

    def over_x(rel, h, i):
        at = piece(at_x(SIDE - rel), True, h, i)
        if rel == 2:
            got(at, xf_r.at[h, i])
        else:
            k = rel // 2
            got(at, xh_r.at[k, h, i])
            if h == k:
                send(at, at, s_x, xf_r.at[h, i], dev_x(1 + 2 * k))
        send(at, at, s_x, zx_r.at[rel - 1, h, i], dev_z(1 if h == 0 else n_z - 1))
        send(at, at, s_x, dd_r.at[rel], partner)

    def over_z(rel, h, i):
        at = piece(at_x(SIDE - rel), False, h, i)
        got(at, zx_r.at[rel - 1, h, i])
        send(at, at, s_x, dd_r.at[rel], partner)

    got_quarter(1)
    for h in range(2):
        got(unit(y, 2, h), sf_r.at[h])
        spread(2, h)
    onward(0)
    onward(1)
    over_x(1, 0, 0)
    over_x(3, 1, 0)
    got(G.at[e, 0:3], g_r.at[0])
    send(G.at[e], G.at[e], s_gd, g_r.at[1], partner)
    onward(3)
    over_x(1, 0, 1)
    over_x(3, 1, 1)
    over_z(1, 0, 0)
    over_z(3, 1, 0)
    onward(2)
    over_x(1, 1, 0)
    over_x(3, 0, 0)
    over_z(1, 0, 1)
    over_z(3, 1, 1)
    over_x(1, 1, 1)
    over_x(3, 0, 1)
    over_z(3, 0, 0)
    over_z(1, 1, 0)
    over_x(2, 0, 0)
    over_x(2, 1, 0)
    over_z(3, 0, 1)
    over_z(1, 1, 1)
    over_x(2, 0, 1)
    over_x(2, 1, 1)
    got(W.at[0:8], wrest.at[0])
    got(G.at[1 - e], g_r.at[1])

    n_acc = acc.shape[1]
    cut = n_acc // 2
    step = 32

    def tokens_of(a):
        return pl.ds(pl.multiple_of(a * 2 * tok, 2 * tok), 2 * tok)

    def weights(lo, hi, slabs=range(SIDE * SIDE)):
        return jnp.concatenate([W[k, lo:hi].reshape((hi - lo) * q, lanes) for k in slabs], axis=1)

    def turn(rel):
        ST[rel] = S[:, tokens_of(at_x(SIDE - rel))].T

    def forward(rel, before=None):
        a = at_x(SIDE - rel)
        got(X.at[:, a, 1 - e], dd_r.at[rel])
        if before is not None:
            turn(before)

        def both(i):
            return X[i, a].reshape(2 * tok, width)

        C[0 : 2 * q, :] = mm(weights(0, 2), both(0), NT)
        C[2 * q : 4 * q, :] = mm(weights(3, 5), both(0), NT)
        C[4 * q : 6 * q, :] = mm(weights(0, 2), both(1), NT)
        C[6 * q : 7 * q, :] = mm(weights(2, 3), both(2), NT)
        C[7 * q : 8 * q, :] = mm(weights(5, 6), both(2), NT)
        gate = jnp.concatenate([G[0, a, pl.ds(e, 1), :], G[1, a, pl.ds(e, 1), :]], axis=1)
        cols = tokens_of(a)

        def rows_of(i, carry):
            at = pl.multiple_of(i * step, step)

            def c(k):
                return C[pl.ds(k * q + at, step), :]

            pre, up = c(0), c(1)
            pre_dot, up_dot = c(4) + c(2), c(5) + c(3)
            g, g_dot = c(6) * gate, c(7) * gate
            sigma = jax.nn.sigmoid(pre)
            rest = 1.0 - sigma
            s0 = pre * sigma
            s1 = sigma * (1.0 + pre * rest)
            s2 = sigma * rest * (2.0 + pre * (1.0 - 2.0 * sigma))
            S[pl.ds(at, step), cols] = (
                g_dot * up * s1 + g * up_dot * s1 + g * up * s2 * pre_dot
            ).astype(BF16)
            S[pl.ds(q + at, step), cols] = (g_dot * s0 + g * s1 * pre_dot).astype(BF16)
            S[pl.ds(2 * q + at, step), cols] = (g * up * s1).astype(BF16)
            S[pl.ds(3 * q + at, step), cols] = (g * s0).astype(BF16)
            H[pl.ds(at, step), cols] = ((s1 * pre_dot * up + s0 * up_dot) * gate).astype(BF16)
            return carry

        lax.fori_loop(0, q // step, rows_of, 0)

    def tokens_back(n, rels):
        slabs = range(SIDE * n, SIDE * n + SIDE)
        for rel in rels:
            left = jnp.concatenate(
                [ST[rel, pl.ds(pl.multiple_of(k * tok, tok), tok), :] for k in (e, 1 - e)], axis=0
            )
            value = mm(left[:, 0 : 2 * q], weights(0, 2, slabs)) + mm(left[:, 2 * q : 4 * q], weights(3, 5, slabs))
            Pown[rel, n] = value[0:tok]
            PDs[rel, n] = value[tok : 2 * tok].astype(BF16)
            send(PDs.at[rel, n], PDr.at[rel, n], s_pd, pd_r.at[rel, n], partner)

    def weights_back(n):
        cols = pl.ds(pl.multiple_of(n * part, part), part)

        def every(i):
            return X[i, :, :, :, cols].reshape(SIDE * 2 * tok, part)

        acc[n, 0 : 2 * q, :] = mm(S[2 * q : 4 * q, :], every(1)) + mm(S[0 : 2 * q, :], every(0))
        acc[n, 2 * q : 3 * q, :] = mm(H[...], every(2))

    def summed(rel, n, h):
        at = pl.ds(h * half, half)
        return Pown[rel, n, at, :] + PDr[rel, n, at, :].astype(F32)

    def acc_half(k, h):
        return acc[k, h * cut : (h + 1) * cut, :]

    def x_first(n):
        for rel in (2, 1, 3):
            got(PDr.at[rel, n], pd_r.at[rel, n])
            if rel == 2:
                for h in range(2):
                    xopp[n, h] = summed(2, n, h).astype(BF16)
                    send(xopp.at[n, h], xropp.at[n, h], s_xo, xo_r.at[n, h], dev_x(1 + 2 * h))
            else:
                k, h = (1, 0) if rel == 1 else (0, 1)
                xs[n, k, h] = summed(rel, n, h).astype(BF16)
                send(xs.at[n, k, h], xr.at[n, k, h], s_xs, xp_r.at[n], dev_x(1 + 2 * k))

    def x_second(n):
        for k in range(2):
            got(xropp.at[n, k], xo_r.at[n, k])
            xs[n, k, k] = (summed(3 - 2 * k, n, k) + xropp[n, k].astype(F32)).astype(BF16)
            send(xs.at[n, k, k], xr.at[n, k, k], s_xs, xp_r.at[n], dev_x(1 + 2 * k))

    piece_z = tok // n_z

    def at_z(d):
        return lax.rem(t + d + n_z, n_z)

    mid = part // 2

    def lane_half(h):
        return slice(h * mid, (h + 1) * mid)

    def z_scatter(n):
        got(PDr.at[0, n], pd_r.at[0, n])
        got(xr.at[n], xp_r.at[n])
        for h in range(2):
            total = summed(0, n, h) + xr[n, 0, h].astype(F32) + xr[n, 1, h].astype(F32)
            total = total.reshape(n_z // 2, piece_z, part)
            at = pl.ds(h * (n_z // 2), n_z // 2)
            Zt[n, at] = total
            Zs[n, at] = total.astype(BF16)
        for k in range(2):
            far = at_z(3 - 6 * k)
            send(Zs.at[n, far], Z3.at[n, k, :, 0:part], s_z, z1_r.at[n, k], dev_z(2 + (n_z - 4) * k))
            src = Zs.at[n, at_z(4), :, lane_half(k)]
            send(src, Z3.at[n, k, :, part:], s_z, z1_r.at[n, k], dev_z(2 + (n_z - 4) * k))

    def z_middle(n):
        for k in range(2):
            sign = 1 - 2 * k
            got(Z3.at[n, k], z1_r.at[n, k])
            Zm[n, 0, k] = (Zt[n, at_z(sign)] + Z3[n, k, :, 0:part].astype(F32)).astype(BF16)
            send(Zm.at[n, 0, k], Zr.at[n, 0, k], s_z, z4_r.at[n], dev_z((sign + n_z) % n_z))
            here, there = lane_half(k), lane_half(1 - k)
            next_but_one = at_z(2 * sign)
            Zm[n, 1, k, :, here] = (Zt[n, next_but_one, :, here] + Z3[n, k, :, part:].astype(F32)).astype(BF16)
            Zm[n, 1, k, :, there] = Zt[n, next_but_one, :, there].astype(BF16)
            send(Zm.at[n, 1, k], Zr.at[n, 1, k], s_z, z4_r.at[n], dev_z((2 * sign + n_z) % n_z))

    def z_gather(n):
        done = Zt[n, t]
        got(Zr.at[n], z4_r.at[n])
        for i in range(2):
            for k in range(2):
                done += Zr[n, i, k].astype(F32)
        Zf[n, t] = done.astype(BF16)
        for i in (1, 0):
            for k in range(2):
                d = (i + 1) * (1 - 2 * k)
                sem = (zd_r if i == 0 else z2_r).at[n]
                send(Zf.at[n, t], Zf.at[n, t], s_z, sem, dev_z((d + n_z) % n_z))

    def z_relay(n):
        got(Zf.at[n, 0:2], z2_r.at[n])
        for k in range(2):
            sign = 1 - 2 * k
            src = at_z(-2 * sign)
            send(Zf.at[n, src], Zf.at[n, src], s_z, zd_r.at[n], dev_z((sign + n_z) % n_z))
            at = Zf.at[n, src, :, lane_half(k)]
            send(at, at, s_z, zd_r.at[n], dev_z((2 * sign + n_z) % n_z))

    def z_done(n):
        got(Zf.at[n, 0:5], zd_r.at[n])
        pltpu.make_async_copy(Zf.at[n], out_tok.at[:, :, n * part : (n + 1) * part], loc.at[3]).start()

    def y_first():
        weights_back(at_y(2))
        for h in range(2):
            yopp[h] = acc_half(at_y(2), h).astype(BF16)
            send(yopp.at[h], yropp.at[h], s_yo, yo_r.at[h], dev_y(1 + 2 * h))

    def y_next(k):
        h = 1 - k
        weights_back(at_y(1 + 2 * k))
        ys[k, h] = acc_half(at_y(1 + 2 * k), h).astype(BF16)
        send(ys.at[k, h], yr.at[k, h], s_ys, yp_r.at[k, h], dev_y(1 + 2 * k))

    def y_second():
        for k in range(2):
            got(yropp.at[k], yo_r.at[k])
            ys[k, k] = (acc_half(at_y(1 + 2 * k), k) + yropp[k].astype(F32)).astype(BF16)
            send(ys.at[k, k], yr.at[k, k], s_ys, yp_r.at[k, k], dev_y(1 + 2 * k))

    def x_slices():
        for h in range(2):
            for k in range(2):
                got(yr.at[k, h], yp_r.at[k, h])
            value = acc_half(y, h) + yr[0, h].astype(F32) + yr[1, h].astype(F32)
            value = value.astype(BF16)
            for k in range(SIDE):
                R[h, k] = value[:, k * lanes : (k + 1) * lanes]
            OUT[x, h] = R[h, x]
            for d in (1, 3, 2):
                send(R.at[h, at_x(d)], OUT.at[x, h], s_r, ra_r.at[0], dev_x(d))

    def weights_out():
        got(OUT.at[0:3], ra_r.at[0])
        for k in range(SIDE):
            first, rest = k * q, n_acc - cut - q
            for src, dst in (
                (OUT.at[k, 0, 0:q], out_in.at[0, first : first + q]),
                (OUT.at[k, 0, q:cut], out_in.at[1, first : first + cut - q]),
                (OUT.at[k, 1, 0:rest], out_in.at[1, first + cut - q : first + q]),
                (OUT.at[k, 1, rest:cut], out_out.at[first : first + q]),
            ):
                pltpu.make_async_copy(src, dst, loc.at[4]).start()

    forward(0)
    over_z(2, 0, 0)
    over_z(2, 1, 0)
    forward(1, 0)
    over_z(2, 0, 1)
    over_z(2, 1, 1)
    forward(3, 1)
    forward(2, 3)
    turn(2)
    far = (2, 1, 3)
    tokens_back(0, far)
    x_first(0)
    y_first()
    tokens_back(1, far)
    x_first(1)
    x_second(0)
    tokens_back(2, far)
    x_first(2)
    x_second(1)
    y_next(0)
    tokens_back(3, far)
    x_first(3)
    y_next(1)
    tokens_back(0, (0,))
    x_second(2)
    z_scatter(0)
    tokens_back(1, (0,))
    z_scatter(1)
    x_second(3)
    y_second()
    tokens_back(2, (0,))
    z_middle(0)
    z_scatter(2)
    tokens_back(3, (0,))
    weights_back(y)
    z_middle(1)
    z_gather(0)
    z_scatter(3)
    z_middle(2)
    z_gather(1)
    z_relay(0)
    x_slices()
    z_middle(3)
    z_gather(2)
    z_relay(1)
    z_gather(3)
    z_relay(2)
    z_done(0)
    z_done(1)
    weights_out()
    z_relay(3)
    z_done(2)
    z_done(3)
    for ref, sem in (
        (W, s_w), (X.at[:, :, :, 0 : tok - tok // 8, :], s_x), (PDs, s_pd), (xopp, s_xo), (xs, s_xs), (yopp, s_yo),
        (ys, s_ys), (R.at[:, 0:3], s_r), (Zt.at[:, 0:7], s_z), (G.at[0, 0:3], s_g), (G.at[0], s_gd),
    ):
        sent(ref, sem)
    got(OUT, loc.at[4])
    got(Zf, loc.at[3])


def widen_kernel(*refs):
    for src, dst in zip(refs[:3], refs[3:]):
        dst[...] = src[...].astype(F32)


def widen(tok, w_in, w_out):
    steps = 4
    specs = [
        pl.BlockSpec((tok.shape[0] // steps, tok.shape[1]), lambda i: (i, 0)),
        pl.BlockSpec((2, w_in.shape[1] // steps, w_in.shape[2]), lambda i: (0, i, 0)),
        pl.BlockSpec((w_out.shape[0] // steps, w_out.shape[1]), lambda i: (i, 0)),
    ]
    return pl.pallas_call(
        widen_kernel,
        grid=(steps,),
        in_specs=specs,
        out_specs=specs,
        out_shape=[jax.ShapeDtypeStruct(a.shape, F32) for a in (tok, w_in, w_out)],
    )(tok, w_in, w_out)


def shards(n_z, tokens, tangent, cotangent, expert_ids, gates, w_in, v_in, w_out, v_out):
    tok = tokens.shape[0]
    ff, lanes = w_in.shape[2:]
    width = tokens.shape[1]
    q = ff // SIDE
    half = tok // 2
    part = width // SIDE
    cut = 3 * q // 2
    dma = pltpu.SemaphoreType.DMA
    vmem = pl.BlockSpec(memory_space=pltpu.VMEM)
    hbm = pl.BlockSpec(memory_space=pltpu.HBM)
    y_tok, y_in, y_out = pl.pallas_call(
        functools.partial(kernel, n_z),
        out_shape=(
            jax.ShapeDtypeStruct((n_z, tok // n_z, width), BF16),
            jax.ShapeDtypeStruct((2, ff, lanes), BF16),
            jax.ShapeDtypeStruct((ff, lanes), BF16),
        ),
        in_specs=[vmem, vmem] + [hbm] * 7,
        out_specs=(hbm, hbm, hbm),
        scratch_shapes=[
            pltpu.VMEM((SIDE * SIDE, 6, q, lanes), BF16),
            pltpu.VMEM((6, ff, lanes), BF16),
            pltpu.VMEM((2, 3, q, lanes), BF16),
            pltpu.VMEM((3, SIDE, 2, tok, width), BF16),
            pltpu.VMEM((2, SIDE, 8, tok), F32),
            pltpu.VMEM((8 * q, 2 * tok), F32),
            pltpu.VMEM((4 * q, SIDE * 2 * tok), BF16),
            pltpu.VMEM((4, 2 * tok, 4 * q), BF16),
            pltpu.VMEM((q, SIDE * 2 * tok), BF16),
            pltpu.VMEM((SIDE, 3 * q, part), F32),
            pltpu.VMEM((4, SIDE, tok, part), F32),
            pltpu.VMEM((4, SIDE, tok, part), BF16),
            pltpu.VMEM((4, SIDE, tok, part), BF16),
            pltpu.VMEM((SIDE, 2, 2, half, part), BF16),
            pltpu.VMEM((SIDE, 2, half, part), BF16),
            pltpu.VMEM((SIDE, 2, 2, half, part), BF16),
            pltpu.VMEM((SIDE, 2, half, part), BF16),
            pltpu.VMEM((2, 2, cut, part), BF16),
            pltpu.VMEM((2, cut, part), BF16),
            pltpu.VMEM((2, 2, cut, part), BF16),
            pltpu.VMEM((2, cut, part), BF16),
            pltpu.VMEM((2, SIDE, cut, lanes), BF16),
            pltpu.VMEM((SIDE, 2, cut, lanes), BF16),
            pltpu.VMEM((SIDE, n_z, tok // n_z, part), F32),
            pltpu.VMEM((SIDE, n_z, tok // n_z, part), BF16),
            pltpu.VMEM((SIDE, 2, tok // n_z, part + part // 2), BF16),
            pltpu.VMEM((SIDE, 2, 2, tok // n_z, part), BF16),
            pltpu.VMEM((SIDE, 2, 2, tok // n_z, part), BF16),
            pltpu.VMEM((SIDE, n_z, tok // n_z, part), BF16),
            dma((5,)),
            dma((11,)),
            dma((2, 2)), dma((2,)), dma((2,)),
            dma((2, 4)), dma((1,)),
            dma((2, 2, 2)), dma((2, 2)), dma((3, 2, 2)),
            dma((2,)), dma((4,)), dma((4, 4)),
            dma((4, 2)), dma((4,)),
            dma((2,)), dma((2, 2)), dma((1,)),
            dma((4, 2)), dma((4,)), dma((4,)), dma((4,)),
        ],
        compiler_params=pltpu.CompilerParams(
            collective_id=0, has_side_effects=True, vmem_limit_bytes=62 * 1024 * 1024
        ),
    )(
        expert_ids.T, gates.T, tokens, tangent, cotangent, w_in[0], v_in[0], w_out[0], v_out[0]
    )
    y_tok, y_in, y_out = widen(y_tok.reshape(tok, width), y_in, y_out)
    return y_tok, y_in[None], y_out[None]


def solution(mesh):
    rows = P(("expert", "dp"), None)
    w_spec = P(("tensor", "expert"), None, None, "dp")
    o_spec = P(("tensor", "expert"), None, "dp")
    return jax.shard_map(
        functools.partial(shards, mesh.shape["tensor"]),
        mesh=mesh,
        in_specs=(rows,) * 5 + (w_spec, w_spec, o_spec, o_spec),
        out_specs=(rows, w_spec, o_spec),
        check_vma=False,
    )
```

```python
import functools

import jax
import jax.numpy as jnp
from jax import lax
from jax.experimental import pallas as pl
from jax.experimental.pallas import tpu as pltpu
from jax.sharding import PartitionSpec as P

MESH = pl.DeviceIdType.MESH
F32 = jnp.float32
BF16 = jnp.bfloat16
SIDE = 4
NT = (((1,), (1,)), ((), ()))
NN = (((1,), (0,)), ((), ()))


def mm(a, b, dims=NN):
    return lax.dot_general(a, b, dims, preferred_element_type=F32)


def kernel(
    n_z, ids_ref, gates_ref, tok_ref, tan_ref, cot_ref, wi_ref, vi_ref, wo_ref, vo_ref,
    out_tok, out_in, out_out,
    W, Wsrc, stage, X, G, C, S, ST, H, acc, Pown, PDs, PDr, xs, xopp, xr, xropp, ys, yopp, yr, yropp, R, OUT, Zt, Zs, Z3, Zm, Zr, Zf,
    loc, snd, wa_r, st_r, sf_r, wy_r, wrest, xh_r, xf_r, zx_r, g_r, dd_r, pd_r, xo_r, xp_r, yo_r, yp_r, ra_r,
    z1_r, z4_r, z2_r, zd_r,
):
    t = lax.axis_index("tensor")
    e = lax.axis_index("expert")
    p = lax.axis_index("dp")
    y, x = p // SIDE, p % SIDE
    color = lax.rem(t, 2)
    tok = tok_ref.shape[0]
    half = tok // 2
    quarter = tok // 4
    lanes = wi_ref.shape[-1]
    q = W.shape[2]
    width = tok_ref.shape[1]
    part = width // SIDE

    def at_x(d):
        return lax.rem(x + d, SIDE)

    def at_y(d):
        return lax.rem(y + d, SIDE)

    def dev_x(d):
        return (t, e, y * SIDE + at_x(d))

    def dev_y(d):
        return (t, e, at_y(d) * SIDE + x)

    def dev_z(d):
        return (lax.rem(t + d, n_z), e, p)

    partner = (t, 1 - e, p)
    s_w, s_x, s_pd, s_xo, s_xs, s_yo, s_ys, s_r, s_z, s_g, s_gd = (snd.at[i] for i in range(11))

    def send(src, dst, ssem, rsem, dev):
        pltpu.make_async_remote_copy(
            src_ref=src, dst_ref=dst, send_sem=ssem, recv_sem=rsem, device_id=dev, device_id_type=MESH
        ).start()

    def got(ref, rsem):
        pltpu.make_async_remote_copy(
            src_ref=ref, dst_ref=ref, send_sem=s_w, recv_sem=rsem, device_id=partner, device_id_type=MESH
        ).wait_recv()

    def sent(ref, ssem):
        pltpu.make_async_remote_copy(
            src_ref=ref, dst_ref=ref, send_sem=ssem, recv_sem=ssem, device_id=partner, device_id_type=MESH
        ).wait_send()

    barrier = pltpu.get_barrier_semaphore()
    peers = [partner] + [dev_x(d) for d in (1, 2, 3)] + [dev_y(d) for d in (1, 3)] + [dev_z(d) for d in (1, 2, n_z - 2, n_z - 1)]
    for peer in peers:
        pl.semaphore_signal(barrier, inc=1, device_id=peer, device_id_type=MESH)

    def rows(k):
        return pl.ds(pl.multiple_of(k * q, q), q)

    for src, dst, i in (
        (wi_ref, Wsrc.at[0:2], 0),
        (wo_ref, Wsrc.at[2], 0),
        (vi_ref, Wsrc.at[3:5], 0),
        (vo_ref, Wsrc.at[5], 0),
        (wi_ref.at[:, rows(x), :], W.at[p, 0:2], 1),
        (wo_ref.at[rows(x), :], W.at[p, 2], 1),
        (vi_ref.at[:, rows(x), :], W.at[p, 3:5], 1),
        (vo_ref.at[rows(x), :], W.at[p, 5], 1),
        (tok_ref, X.at[0, x, e], 2),
        (tan_ref, X.at[1, x, e], 2),
        (cot_ref, X.at[2, x, e], 2),
    ):
        pltpu.make_async_copy(src, dst, loc.at[i]).start()
    ids, gates = ids_ref[...], gates_ref[...]
    for r in range(2):
        G[e, x, pl.ds(r, 1), :] = jnp.sum(jnp.where(ids == 2 * t + r, gates, 0.0), axis=0, keepdims=True)
    pl.semaphore_wait(barrier, len(peers))

    got(Wsrc, loc.at[0])

    def quarter_of(h, k):
        return Wsrc.at[3 * h : 3 * h + 3, rows(k), :]

    def unit(yy, d, h):
        return W.at[yy * SIDE + at_x(SIDE - d), 3 * h : 3 * h + 3]

    def quarter_to(h):
        for k, d in enumerate((1, 3)):
            send(quarter_of(h, at_x(d)), unit(y, 0, h), s_w, wa_r.at[k, h], dev_x(d))

    quarter_to(0)
    for h in range(2):
        send(quarter_of(h, at_x(2)), stage.at[h], s_w, st_r.at[h], dev_x(1 + 2 * h))
    quarter_to(1)
    for d in (1, 3, 2):
        send(G.at[e, x], G.at[e, x], s_g, g_r.at[0], dev_x(d))
    got(W.at[p], loc.at[1])

    order = (0, 1, 3, 2)

    def spread(d, h):
        k = order.index(d)
        for i in range(2):
            sem = wy_r.at[i, k] if i == h else wrest.at[1]
            send(unit(y, d, h), unit(y, d, h), s_w, sem, dev_y(1 + 2 * i))

    def onward(d):
        k = order.index(d)
        for h in range(2):
            at = unit(at_y(3 - 2 * h), d, h)
            got(at, wy_r.at[h, k])
            send(at, at, s_w, wrest.at[0], dev_y(1 + 2 * h))

    def got_quarter(h):
        for k, d in enumerate((1, 3)):
            got(unit(y, d, h), wa_r.at[k, h])
            spread(d, h)

    spread(0, 0)
    spread(0, 1)
    got(X.at[:, x, e], loc.at[2])

    def piece(a, own, h, i):
        eighth = quarter // 2
        first = (color if own else 1 - color) * half + h * quarter + i * eighth
        return X.at[:, a, e, pl.ds(pl.multiple_of(first, eighth), eighth), :]

    def over_links(k, h, i):
        at = piece(x, True, h, i)
        send(at, at, s_x, xh_r.at[k, h, i], dev_x(1 + 2 * k))

    over_links(0, 0, 0)
    over_links(1, 1, 0)
    send(X.at[:, x, e], X.at[:, x, e], s_x, dd_r.at[0], partner)
    got_quarter(0)
    for h in range(2):
        got(stage.at[h], st_r.at[h])
        send(stage.at[h], unit(y, 1 + 2 * h, h), s_w, sf_r.at[h], dev_x(1 + 2 * h))
    for k, h, i in ((0, 0, 1), (1, 1, 1), (0, 1, 0), (1, 0, 0), (0, 1, 1), (1, 0, 1)):
        over_links(k, h, i)

    def over_x(rel, h, i):
        at = piece(at_x(SIDE - rel), True, h, i)
        if rel == 2:
            got(at, xf_r.at[h, i])
        else:
            k = rel // 2
            got(at, xh_r.at[k, h, i])
            if h == k:
                send(at, at, s_x, xf_r.at[h, i], dev_x(1 + 2 * k))
        send(at, at, s_x, zx_r.at[rel - 1, h, i], dev_z(1 if h == 0 else n_z - 1))
        send(at, at, s_x, dd_r.at[rel], partner)

    def over_z(rel, h, i):
        at = piece(at_x(SIDE - rel), False, h, i)
        got(at, zx_r.at[rel - 1, h, i])
        send(at, at, s_x, dd_r.at[rel], partner)

    n_acc = acc.shape[1]
    cut = n_acc // 2
    step = 32

    def tokens_of(a):
        return pl.ds(pl.multiple_of(a * 2 * tok, 2 * tok), 2 * tok)

    def weights(lo, hi, slabs=range(SIDE * SIDE)):
        return jnp.concatenate([W[k, lo:hi].reshape((hi - lo) * q, lanes) for k in slabs], axis=1)

    def turn(rel):
        ST[rel] = S[:, tokens_of(at_x(SIDE - rel))].T

    def products(rel, quarters, add):
        a = at_x(SIDE - rel)
        if not add:
            got(X.at[:, a, 1 - e], dd_r.at[rel])
        slabs = [at_y(d) * SIDE + k for d in quarters for k in range(SIDE)]
        for first, lo, hi, i in ((0, 0, 2, 0), (2, 3, 5, 0), (4, 0, 2, 1), (6, 2, 3, 2), (7, 5, 6, 2)):
            cols = [pl.ds(pl.multiple_of(at_y(d) * part, part), part) for d in quarters]
            right = jnp.concatenate([X[i, a, :, :, c].reshape(2 * tok, part) for c in cols], axis=1)
            value = mm(weights(lo, hi, slabs), right, NT)
            at = slice(first * q, (first + hi - lo) * q)
            C[rel, at, :] = C[rel, at, :] + value if add else value

    def forward(rel, before=None):
        a = at_x(SIDE - rel)
        if before is not None:
            turn(before)
        products(rel, (2,) if rel == 0 else (0, 1, 3, 2), rel == 0)
        gate = jnp.concatenate([G[0, a, pl.ds(e, 1), :], G[1, a, pl.ds(e, 1), :]], axis=1)
        cols = tokens_of(a)

        def rows_of(i, carry):
            at = pl.multiple_of(i * step, step)

            def c(k):
                return C[rel, pl.ds(k * q + at, step), :]

            pre, up = c(0), c(1)
            pre_dot, up_dot = c(4) + c(2), c(5) + c(3)
            g, g_dot = c(6) * gate, c(7) * gate
            sigma = jax.nn.sigmoid(pre)
            rest = 1.0 - sigma
            s0 = pre * sigma
            s1 = sigma * (1.0 + pre * rest)
            s2 = sigma * rest * (2.0 + pre * (1.0 - 2.0 * sigma))
            S[pl.ds(at, step), cols] = (
                g_dot * up * s1 + g * up_dot * s1 + g * up * s2 * pre_dot
            ).astype(BF16)
            S[pl.ds(q + at, step), cols] = (g_dot * s0 + g * s1 * pre_dot).astype(BF16)
            S[pl.ds(2 * q + at, step), cols] = (g * up * s1).astype(BF16)
            S[pl.ds(3 * q + at, step), cols] = (g * s0).astype(BF16)
            H[pl.ds(at, step), cols] = ((s1 * pre_dot * up + s0 * up_dot) * gate).astype(BF16)
            return carry

        lax.fori_loop(0, q // step, rows_of, 0)

    def tokens_back(n, rels):
        slabs = range(SIDE * n, SIDE * n + SIDE)
        for rel in rels:
            left = jnp.concatenate(
                [ST[rel, pl.ds(pl.multiple_of(k * tok, tok), tok), :] for k in (e, 1 - e)], axis=0
            )
            value = mm(left[:, 0 : 2 * q], weights(0, 2, slabs)) + mm(left[:, 2 * q : 4 * q], weights(3, 5, slabs))
            Pown[rel, n] = value[0:tok]
            PDs[rel, n] = value[tok : 2 * tok].astype(BF16)
            send(PDs.at[rel, n], PDr.at[rel, n], s_pd, pd_r.at[rel, n], partner)

    def weights_back(n):
        cols = pl.ds(pl.multiple_of(n * part, part), part)

        def every(i):
            return X[i, :, :, :, cols].reshape(SIDE * 2 * tok, part)

        acc[n, 0 : 2 * q, :] = mm(S[2 * q : 4 * q, :], every(1)) + mm(S[0 : 2 * q, :], every(0))
        acc[n, 2 * q : 3 * q, :] = mm(H[...], every(2))

    def summed(rel, n, h):
        at = pl.ds(h * half, half)
        return Pown[rel, n, at, :] + PDr[rel, n, at, :].astype(F32)

    def acc_half(k, h):
        return acc[k, h * cut : (h + 1) * cut, :]

    def x_far(n):
        got(PDr.at[2, n], pd_r.at[2, n])
        for h in range(2):
            xopp[n, h] = summed(2, n, h).astype(BF16)
            send(xopp.at[n, h], xropp.at[n, h], s_xo, xo_r.at[n, h], dev_x(1 + 2 * h))

    def x_near(n):
        for rel, k, h in ((1, 1, 0), (3, 0, 1)):
            got(PDr.at[rel, n], pd_r.at[rel, n])
            xs[n, k, h] = summed(rel, n, h).astype(BF16)
            send(xs.at[n, k, h], xr.at[n, k, h], s_xs, xp_r.at[n], dev_x(1 + 2 * k))

    def x_second(n):
        for k in range(2):
            got(xropp.at[n, k], xo_r.at[n, k])
            xs[n, k, k] = (summed(3 - 2 * k, n, k) + xropp[n, k].astype(F32)).astype(BF16)
            send(xs.at[n, k, k], xr.at[n, k, k], s_xs, xp_r.at[n], dev_x(1 + 2 * k))

    piece_z = tok // n_z

    def at_z(d):
        return lax.rem(t + d + n_z, n_z)

    mid = part // 2

    def lane_half(h):
        return slice(h * mid, (h + 1) * mid)

    def z_scatter(n):
        got(PDr.at[0, n], pd_r.at[0, n])
        got(xr.at[n], xp_r.at[n])
        for h in range(2):
            total = summed(0, n, h) + xr[n, 0, h].astype(F32) + xr[n, 1, h].astype(F32)
            total = total.reshape(n_z // 2, piece_z, part)
            at = pl.ds(h * (n_z // 2), n_z // 2)
            Zt[n, at] = total
            Zs[n, at] = total.astype(BF16)
        for k in range(2):
            far = at_z(3 - 6 * k)
            send(Zs.at[n, far], Z3.at[n, k, :, 0:part], s_z, z1_r.at[n, k], dev_z(2 + (n_z - 4) * k))
            src = Zs.at[n, at_z(4), :, lane_half(k)]
            send(src, Z3.at[n, k, :, part:], s_z, z1_r.at[n, k], dev_z(2 + (n_z - 4) * k))

    def z_middle(n):
        for k in range(2):
            sign = 1 - 2 * k
            got(Z3.at[n, k], z1_r.at[n, k])
            Zm[n, 0, k] = (Zt[n, at_z(sign)] + Z3[n, k, :, 0:part].astype(F32)).astype(BF16)
            send(Zm.at[n, 0, k], Zr.at[n, 0, k], s_z, z4_r.at[n], dev_z((sign + n_z) % n_z))
            here, there = lane_half(k), lane_half(1 - k)
            next_but_one = at_z(2 * sign)
            Zm[n, 1, k, :, here] = (Zt[n, next_but_one, :, here] + Z3[n, k, :, part:].astype(F32)).astype(BF16)
            Zm[n, 1, k, :, there] = Zt[n, next_but_one, :, there].astype(BF16)
            send(Zm.at[n, 1, k], Zr.at[n, 1, k], s_z, z4_r.at[n], dev_z((2 * sign + n_z) % n_z))

    def z_gather(n):
        done = Zt[n, t]
        got(Zr.at[n], z4_r.at[n])
        for i in range(2):
            for k in range(2):
                done += Zr[n, i, k].astype(F32)
        Zf[n, t] = done.astype(BF16)
        for i in (1, 0):
            for k in range(2):
                d = (i + 1) * (1 - 2 * k)
                sem = (zd_r if i == 0 else z2_r).at[n]
                send(Zf.at[n, t], Zf.at[n, t], s_z, sem, dev_z((d + n_z) % n_z))

    def z_relay(n):
        got(Zf.at[n, 0:2], z2_r.at[n])
        for k in range(2):
            sign = 1 - 2 * k
            src = at_z(-2 * sign)
            send(Zf.at[n, src], Zf.at[n, src], s_z, zd_r.at[n], dev_z((sign + n_z) % n_z))
            at = Zf.at[n, src, :, lane_half(k)]
            send(at, at, s_z, zd_r.at[n], dev_z((2 * sign + n_z) % n_z))

    def z_done(n):
        got(Zf.at[n, 0:5], zd_r.at[n])
        pltpu.make_async_copy(Zf.at[n], out_tok.at[:, :, n * part : (n + 1) * part], loc.at[3]).start()

    def y_first():
        weights_back(at_y(2))
        for h in range(2):
            yopp[h] = acc_half(at_y(2), h).astype(BF16)
            send(yopp.at[h], yropp.at[h], s_yo, yo_r.at[h], dev_y(1 + 2 * h))

    def y_next(k):
        h = 1 - k
        weights_back(at_y(1 + 2 * k))
        ys[k, h] = acc_half(at_y(1 + 2 * k), h).astype(BF16)
        send(ys.at[k, h], yr.at[k, h], s_ys, yp_r.at[k, h], dev_y(1 + 2 * k))

    def y_second():
        for k in range(2):
            got(yropp.at[k], yo_r.at[k])
            ys[k, k] = (acc_half(at_y(1 + 2 * k), k) + yropp[k].astype(F32)).astype(BF16)
            send(ys.at[k, k], yr.at[k, k], s_ys, yp_r.at[k, k], dev_y(1 + 2 * k))

    def x_slices():
        for h in range(2):
            for k in range(2):
                got(yr.at[k, h], yp_r.at[k, h])
            value = acc_half(y, h) + yr[0, h].astype(F32) + yr[1, h].astype(F32)
            value = value.astype(BF16)
            for k in range(SIDE):
                R[h, k] = value[:, k * lanes : (k + 1) * lanes]
            OUT[x, h] = R[h, x]
            for d in (1, 3, 2):
                send(R.at[h, at_x(d)], OUT.at[x, h], s_r, ra_r.at[0], dev_x(d))

    def weights_out():
        got(OUT.at[0:3], ra_r.at[0])
        for k in range(SIDE):
            first, rest = k * q, n_acc - cut - q
            for src, dst in (
                (OUT.at[k, 0, 0:q], out_in.at[0, first : first + q]),
                (OUT.at[k, 0, q:cut], out_in.at[1, first : first + cut - q]),
                (OUT.at[k, 1, 0:rest], out_in.at[1, first + cut - q : first + q]),
                (OUT.at[k, 1, rest:cut], out_out.at[first : first + q]),
            ):
                pltpu.make_async_copy(src, dst, loc.at[4]).start()

    got_quarter(1)
    for h in range(2):
        got(unit(y, 2, h), sf_r.at[h])
        spread(2, h)
    onward(0)
    onward(1)
    over_x(1, 0, 0)
    over_x(3, 1, 0)
    got(G.at[e, 0:3], g_r.at[0])
    send(G.at[e], G.at[e], s_gd, g_r.at[1], partner)
    onward(3)
    over_x(1, 0, 1)
    over_x(3, 1, 1)
    over_z(1, 0, 0)
    over_z(3, 1, 0)
    onward(2)
    over_x(1, 1, 0)
    over_x(3, 0, 0)
    over_z(1, 0, 1)
    over_z(3, 1, 1)
    got(W.at[0:4], wrest.at[1])
    products(0, (0, 1, 3), False)
    over_x(1, 1, 1)
    over_x(3, 0, 1)
    over_z(3, 0, 0)
    over_z(1, 1, 0)
    over_x(2, 0, 0)
    over_x(2, 1, 0)
    over_z(3, 0, 1)
    over_z(1, 1, 1)
    over_x(2, 0, 1)
    over_x(2, 1, 1)
    got(W.at[0:4], wrest.at[0])
    got(G.at[1 - e], g_r.at[1])
    forward(1)
    over_z(2, 0, 0)
    over_z(2, 1, 0)
    forward(3, 1)
    over_z(2, 0, 1)
    over_z(2, 1, 1)
    forward(0, 3)
    near, far = (1, 3), (2, 1, 3)
    tokens_back(0, near)
    tokens_back(1, near)
    x_near(0)
    forward(2, 0)
    turn(2)
    x_near(1)
    tokens_back(0, (2,))
    tokens_back(1, (2,))
    x_far(0)
    y_first()
    x_far(1)
    tokens_back(0, (0,))
    tokens_back(1, (0,))
    x_second(0)
    tokens_back(2, far)
    x_second(1)
    y_next(0)
    x_far(2)
    x_near(2)
    y_next(1)
    z_scatter(0)
    tokens_back(3, far)
    x_second(2)
    z_scatter(1)
    x_far(3)
    x_near(3)
    z_middle(0)
    y_second()
    tokens_back(2, (0,))
    tokens_back(3, (0,))
    z_middle(1)
    x_second(3)
    z_scatter(2)
    z_gather(0)
    weights_back(y)
    z_gather(1)
    z_middle(2)
    z_scatter(3)
    z_relay(0)
    z_relay(1)
    z_gather(2)
    z_middle(3)
    x_slices()
    z_relay(2)
    z_gather(3)
    z_done(0)
    z_done(1)
    z_relay(3)
    weights_out()
    z_done(2)
    z_done(3)
    for ref, sem in (
        (W, s_w), (X.at[:, :, :, 0 : tok - tok // 8, :], s_x), (PDs, s_pd), (xopp, s_xo), (xs, s_xs), (yopp, s_yo),
        (ys, s_ys), (R.at[:, 0:3], s_r), (Zt.at[:, 0:7], s_z), (G.at[0, 0:3], s_g), (G.at[0], s_gd),
    ):
        sent(ref, sem)
    got(OUT, loc.at[4])
    got(Zf, loc.at[3])


def widen_kernel(*refs):
    for src, dst in zip(refs[:3], refs[3:]):
        dst[...] = src[...].astype(F32)


def widen(tok, w_in, w_out):
    steps = 4
    specs = [
        pl.BlockSpec((tok.shape[0] // steps, tok.shape[1]), lambda i: (i, 0)),
        pl.BlockSpec((2, w_in.shape[1] // steps, w_in.shape[2]), lambda i: (0, i, 0)),
        pl.BlockSpec((w_out.shape[0] // steps, w_out.shape[1]), lambda i: (i, 0)),
    ]
    return pl.pallas_call(
        widen_kernel,
        grid=(steps,),
        in_specs=specs,
        out_specs=specs,
        out_shape=[jax.ShapeDtypeStruct(a.shape, F32) for a in (tok, w_in, w_out)],
    )(tok, w_in, w_out)


def shards(n_z, tokens, tangent, cotangent, expert_ids, gates, w_in, v_in, w_out, v_out):
    tok = tokens.shape[0]
    ff, lanes = w_in.shape[2:]
    width = tokens.shape[1]
    q = ff // SIDE
    half = tok // 2
    part = width // SIDE
    cut = 3 * q // 2
    dma = pltpu.SemaphoreType.DMA
    vmem = pl.BlockSpec(memory_space=pltpu.VMEM)
    hbm = pl.BlockSpec(memory_space=pltpu.HBM)
    y_tok, y_in, y_out = pl.pallas_call(
        functools.partial(kernel, n_z),
        out_shape=(
            jax.ShapeDtypeStruct((n_z, tok // n_z, width), BF16),
            jax.ShapeDtypeStruct((2, ff, lanes), BF16),
            jax.ShapeDtypeStruct((ff, lanes), BF16),
        ),
        in_specs=[vmem, vmem] + [hbm] * 7,
        out_specs=(hbm, hbm, hbm),
        scratch_shapes=[
            pltpu.VMEM((SIDE * SIDE, 6, q, lanes), BF16),
            pltpu.VMEM((6, ff, lanes), BF16),
            pltpu.VMEM((2, 3, q, lanes), BF16),
            pltpu.VMEM((3, SIDE, 2, tok, width), BF16),
            pltpu.VMEM((2, SIDE, 8, tok), F32),
            pltpu.VMEM((4, 8 * q, 2 * tok), F32),
            pltpu.VMEM((4 * q, SIDE * 2 * tok), BF16),
            pltpu.VMEM((4, 2 * tok, 4 * q), BF16),
            pltpu.VMEM((q, SIDE * 2 * tok), BF16),
            pltpu.VMEM((SIDE, 3 * q, part), F32),
            pltpu.VMEM((4, SIDE, tok, part), F32),
            pltpu.VMEM((4, SIDE, tok, part), BF16),
            pltpu.VMEM((4, SIDE, tok, part), BF16),
            pltpu.VMEM((SIDE, 2, 2, half, part), BF16),
            pltpu.VMEM((SIDE, 2, half, part), BF16),
            pltpu.VMEM((SIDE, 2, 2, half, part), BF16),
            pltpu.VMEM((SIDE, 2, half, part), BF16),
            pltpu.VMEM((2, 2, cut, part), BF16),
            pltpu.VMEM((2, cut, part), BF16),
            pltpu.VMEM((2, 2, cut, part), BF16),
            pltpu.VMEM((2, cut, part), BF16),
            pltpu.VMEM((2, SIDE, cut, lanes), BF16),
            pltpu.VMEM((SIDE, 2, cut, lanes), BF16),
            pltpu.VMEM((SIDE, n_z, tok // n_z, part), F32),
            pltpu.VMEM((SIDE, n_z, tok // n_z, part), BF16),
            pltpu.VMEM((SIDE, 2, tok // n_z, part + part // 2), BF16),
            pltpu.VMEM((SIDE, 2, 2, tok // n_z, part), BF16),
            pltpu.VMEM((SIDE, 2, 2, tok // n_z, part), BF16),
            pltpu.VMEM((SIDE, n_z, tok // n_z, part), BF16),
            dma((5,)),
            dma((11,)),
            dma((2, 2)), dma((2,)), dma((2,)),
            dma((2, 4)), dma((2,)),
            dma((2, 2, 2)), dma((2, 2)), dma((3, 2, 2)),
            dma((2,)), dma((4,)), dma((4, 4)),
            dma((4, 2)), dma((4,)),
            dma((2,)), dma((2, 2)), dma((1,)),
            dma((4, 2)), dma((4,)), dma((4,)), dma((4,)),
        ],
        compiler_params=pltpu.CompilerParams(
            collective_id=0, has_side_effects=True, vmem_limit_bytes=62 * 1024 * 1024
        ),
    )(
        expert_ids.T, gates.T, tokens, tangent, cotangent, w_in[0], v_in[0], w_out[0], v_out[0]
    )
    y_tok, y_in, y_out = widen(y_tok.reshape(tok, width), y_in, y_out)
    return y_tok, y_in[None], y_out[None]


def solution(mesh):
    rows = P(("expert", "dp"), None)
    w_spec = P(("tensor", "expert"), None, None, "dp")
    o_spec = P(("tensor", "expert"), None, "dp")
    return jax.shard_map(
        functools.partial(shards, mesh.shape["tensor"]),
        mesh=mesh,
        in_specs=(rows,) * 5 + (w_spec, w_spec, o_spec, o_spec),
        out_specs=(rows, w_spec, o_spec),
        check_vma=False,
    )
```

```python
import functools

import jax
import jax.numpy as jnp
from jax import lax
from jax.experimental import pallas as pl
from jax.experimental.pallas import tpu as pltpu
from jax.sharding import PartitionSpec as P

MESH = pl.DeviceIdType.MESH
F32 = jnp.float32
BF16 = jnp.bfloat16
SIDE = 4
NT = (((1,), (1,)), ((), ()))
NN = (((1,), (0,)), ((), ()))


def mm(a, b, dims=NN):
    return lax.dot_general(a, b, dims, preferred_element_type=F32)


def kernel(
    n_z, ids_ref, gates_ref, tok_ref, tan_ref, cot_ref, wi_ref, vi_ref, wo_ref, vo_ref,
    out_tok, out_in, out_out,
    W, Wsrc, stage, X, G, C, S, ST, H, acc, Pown, PDs, PDr, xs, xopp, xr, xropp, ys, yopp, yr, yropp, R, OUT, Zt, Zs, Z3, Zm, Zr, Zf,
    loc, snd, wa_r, st_r, sf_r, wy_r, wrest, xh_r, xf_r, zx_r, g_r, dd_r, pd_r, xo_r, xp_r, yo_r, yp_r, ra_r,
    z1_r, z4_r, z2_r, zd_r,
):
    t = lax.axis_index("tensor")
    e = lax.axis_index("expert")
    p = lax.axis_index("dp")
    y, x = p // SIDE, p % SIDE
    color = lax.rem(t, 2)
    tok = tok_ref.shape[0]
    half = tok // 2
    quarter = tok // 4
    lanes = wi_ref.shape[-1]
    q = W.shape[2]
    width = tok_ref.shape[1]
    part = width // SIDE

    def at_x(d):
        return lax.rem(x + d, SIDE)

    def at_y(d):
        return lax.rem(y + d, SIDE)

    def dev_x(d):
        return (t, e, y * SIDE + at_x(d))

    def dev_y(d):
        return (t, e, at_y(d) * SIDE + x)

    def dev_z(d):
        return (lax.rem(t + d, n_z), e, p)

    partner = (t, 1 - e, p)
    s_w, s_x, s_pd, s_xo, s_xs, s_yo, s_ys, s_r, s_z, s_g, s_gd = (snd.at[i] for i in range(11))

    def send(src, dst, ssem, rsem, dev):
        pltpu.make_async_remote_copy(
            src_ref=src, dst_ref=dst, send_sem=ssem, recv_sem=rsem, device_id=dev, device_id_type=MESH
        ).start()

    def got(ref, rsem):
        pltpu.make_async_remote_copy(
            src_ref=ref, dst_ref=ref, send_sem=s_w, recv_sem=rsem, device_id=partner, device_id_type=MESH
        ).wait_recv()

    def sent(ref, ssem):
        pltpu.make_async_remote_copy(
            src_ref=ref, dst_ref=ref, send_sem=ssem, recv_sem=ssem, device_id=partner, device_id_type=MESH
        ).wait_send()

    barrier = pltpu.get_barrier_semaphore()
    peers = [partner] + [dev_x(d) for d in (1, 2, 3)] + [dev_y(d) for d in (1, 3)] + [dev_z(d) for d in (1, 2, n_z - 2, n_z - 1)]
    for peer in peers:
        pl.semaphore_signal(barrier, inc=1, device_id=peer, device_id_type=MESH)

    def rows(k):
        return pl.ds(pl.multiple_of(k * q, q), q)

    for src, dst, i in (
        (wi_ref, Wsrc.at[0:2], 0),
        (wo_ref, Wsrc.at[2], 0),
        (vi_ref, Wsrc.at[3:5], 0),
        (vo_ref, Wsrc.at[5], 0),
        (wi_ref.at[:, rows(x), :], W.at[p, 0:2], 1),
        (wo_ref.at[rows(x), :], W.at[p, 2], 1),
        (vi_ref.at[:, rows(x), :], W.at[p, 3:5], 1),
        (vo_ref.at[rows(x), :], W.at[p, 5], 1),
        (tok_ref, X.at[0, x, e], 2),
        (tan_ref, X.at[1, x, e], 2),
        (cot_ref, X.at[2, x, e], 2),
    ):
        pltpu.make_async_copy(src, dst, loc.at[i]).start()
    ids, gates = ids_ref[...], gates_ref[...]
    for r in range(2):
        G[e, x, pl.ds(r, 1), :] = jnp.sum(jnp.where(ids == 2 * t + r, gates, 0.0), axis=0, keepdims=True)
    pl.semaphore_wait(barrier, len(peers))

    got(Wsrc, loc.at[0])

    def quarter_of(h, k):
        return Wsrc.at[3 * h : 3 * h + 3, rows(k), :]

    def unit(yy, d, h):
        return W.at[yy * SIDE + at_x(SIDE - d), 3 * h : 3 * h + 3]

    def quarter_to(h):
        for k, d in enumerate((1, 3)):
            send(quarter_of(h, at_x(d)), unit(y, 0, h), s_w, wa_r.at[k, h], dev_x(d))

    quarter_to(0)
    for h in range(2):
        send(quarter_of(h, at_x(2)), stage.at[h], s_w, st_r.at[h], dev_x(1 + 2 * h))
    quarter_to(1)
    for d in (1, 3, 2):
        send(G.at[e, x], G.at[e, x], s_g, g_r.at[0], dev_x(d))
    got(W.at[p], loc.at[1])

    order = (0, 1, 3, 2)

    def spread(d, h):
        k = order.index(d)
        for i in range(2):
            sem = wy_r.at[i, k] if i == h else wrest.at[1]
            send(unit(y, d, h), unit(y, d, h), s_w, sem, dev_y(1 + 2 * i))

    def onward(d):
        k = order.index(d)
        for h in range(2):
            at = unit(at_y(3 - 2 * h), d, h)
            got(at, wy_r.at[h, k])
            send(at, at, s_w, wrest.at[0], dev_y(1 + 2 * h))

    def got_quarter(h):
        for k, d in enumerate((1, 3)):
            got(unit(y, d, h), wa_r.at[k, h])
            spread(d, h)

    spread(0, 0)
    spread(0, 1)
    got(X.at[:, x, e], loc.at[2])

    def piece(a, own, h, i):
        eighth = quarter // 2
        first = (color if own else 1 - color) * half + h * quarter + i * eighth
        return X.at[:, a, e, pl.ds(pl.multiple_of(first, eighth), eighth), :]

    def over_links(k, h, i):
        at = piece(x, True, h, i)
        send(at, at, s_x, xh_r.at[k, h, i], dev_x(1 + 2 * k))

    over_links(0, 0, 0)
    over_links(1, 1, 0)
    send(X.at[:, x, e], X.at[:, x, e], s_x, dd_r.at[0], partner)
    got_quarter(0)
    for h in range(2):
        got(stage.at[h], st_r.at[h])
        send(stage.at[h], unit(y, 1 + 2 * h, h), s_w, sf_r.at[h], dev_x(1 + 2 * h))
    for k, h, i in ((0, 0, 1), (1, 1, 1), (0, 1, 0), (1, 0, 0), (0, 1, 1), (1, 0, 1)):
        over_links(k, h, i)

    def over_x(rel, h, i):
        at = piece(at_x(SIDE - rel), True, h, i)
        if rel == 2:
            got(at, xf_r.at[h, i])
        else:
            k = rel // 2
            got(at, xh_r.at[k, h, i])
            if h == k:
                send(at, at, s_x, xf_r.at[h, i], dev_x(1 + 2 * k))
        send(at, at, s_x, zx_r.at[rel - 1, h, i], dev_z(1 if h == 0 else n_z - 1))
        send(at, at, s_x, dd_r.at[rel], partner)

    def over_z(rel, h, i):
        at = piece(at_x(SIDE - rel), False, h, i)
        got(at, zx_r.at[rel - 1, h, i])
        send(at, at, s_x, dd_r.at[rel], partner)

    n_acc = acc.shape[1]
    cut = n_acc // 2
    step = 32

    def tokens_of(a):
        return pl.ds(pl.multiple_of(a * 2 * tok, 2 * tok), 2 * tok)

    def weights(lo, hi, slabs=range(SIDE * SIDE)):
        return jnp.concatenate([W[k, lo:hi].reshape((hi - lo) * q, lanes) for k in slabs], axis=1)

    def turn(rel):
        ST[rel] = S[:, tokens_of(at_x(SIDE - rel))].T

    def products(rel, quarters, add):
        a = at_x(SIDE - rel)
        if not add:
            got(X.at[:, a, 1 - e], dd_r.at[rel])
        slabs = [at_y(d) * SIDE + k for d in quarters for k in range(SIDE)]
        for first, lo, hi, i in ((0, 0, 2, 0), (2, 3, 5, 0), (4, 0, 2, 1), (6, 2, 3, 2), (7, 5, 6, 2)):
            cols = [pl.ds(pl.multiple_of(at_y(d) * part, part), part) for d in quarters]
            right = jnp.concatenate([X[i, a, :, :, c].reshape(2 * tok, part) for c in cols], axis=1)
            value = mm(weights(lo, hi, slabs), right, NT)
            at = slice(first * q, (first + hi - lo) * q)
            C[rel, at, :] = C[rel, at, :] + value if add else value

    def forward(rel, before=None):
        a = at_x(SIDE - rel)
        if before is not None:
            turn(before)
        products(rel, (2,) if rel == 0 else (0, 1, 3, 2), rel == 0)
        gate = jnp.concatenate([G[0, a, pl.ds(e, 1), :], G[1, a, pl.ds(e, 1), :]], axis=1)
        cols = tokens_of(a)

        def rows_of(i, carry):
            at = pl.multiple_of(i * step, step)

            def c(k):
                return C[rel, pl.ds(k * q + at, step), :]

            pre, up = c(0), c(1)
            pre_dot, up_dot = c(4) + c(2), c(5) + c(3)
            g, g_dot = c(6) * gate, c(7) * gate
            sigma = jax.nn.sigmoid(pre)
            rest = 1.0 - sigma
            s0 = pre * sigma
            s1 = sigma * (1.0 + pre * rest)
            s2 = sigma * rest * (2.0 + pre * (1.0 - 2.0 * sigma))
            S[pl.ds(at, step), cols] = (
                g_dot * up * s1 + g * up_dot * s1 + g * up * s2 * pre_dot
            ).astype(BF16)
            S[pl.ds(q + at, step), cols] = (g_dot * s0 + g * s1 * pre_dot).astype(BF16)
            S[pl.ds(2 * q + at, step), cols] = (g * up * s1).astype(BF16)
            S[pl.ds(3 * q + at, step), cols] = (g * s0).astype(BF16)
            H[pl.ds(at, step), cols] = ((s1 * pre_dot * up + s0 * up_dot) * gate).astype(BF16)
            return carry

        lax.fori_loop(0, q // step, rows_of, 0)

    def tokens_back(n, rels):
        slabs = range(SIDE * n, SIDE * n + SIDE)
        for rel in rels:
            left = jnp.concatenate(
                [ST[rel, pl.ds(pl.multiple_of(k * tok, tok), tok), :] for k in (e, 1 - e)], axis=0
            )
            value = mm(left[:, 0 : 2 * q], weights(0, 2, slabs)) + mm(left[:, 2 * q : 4 * q], weights(3, 5, slabs))
            Pown[rel, n] = value[0:tok]
            PDs[rel, n] = value[tok : 2 * tok].astype(BF16)
            send(PDs.at[rel, n], PDr.at[rel, n], s_pd, pd_r.at[rel, n], partner)

    def weights_back(n):
        cols = pl.ds(pl.multiple_of(n * part, part), part)

        def every(i):
            return X[i, :, :, :, cols].reshape(SIDE * 2 * tok, part)

        acc[n, 0 : 2 * q, :] = mm(S[2 * q : 4 * q, :], every(1)) + mm(S[0 : 2 * q, :], every(0))
        acc[n, 2 * q : 3 * q, :] = mm(H[...], every(2))

    def summed(rel, n, h):
        at = pl.ds(h * half, half)
        return Pown[rel, n, at, :] + PDr[rel, n, at, :].astype(F32)

    def acc_half(k, h):
        return acc[k, h * cut : (h + 1) * cut, :]

    def x_far(n):
        got(PDr.at[2, n], pd_r.at[2, n])
        for h in range(2):
            xopp[n, h] = summed(2, n, h).astype(BF16)
            send(xopp.at[n, h], xropp.at[n, h], s_xo, xo_r.at[n, h], dev_x(1 + 2 * h))

    def x_near(n):
        for rel, k, h in ((1, 1, 0), (3, 0, 1)):
            got(PDr.at[rel, n], pd_r.at[rel, n])
            xs[n, k, h] = summed(rel, n, h).astype(BF16)
            send(xs.at[n, k, h], xr.at[n, k, h], s_xs, xp_r.at[n], dev_x(1 + 2 * k))

    def x_second(n):
        for k in range(2):
            got(xropp.at[n, k], xo_r.at[n, k])
            xs[n, k, k] = (summed(3 - 2 * k, n, k) + xropp[n, k].astype(F32)).astype(BF16)
            send(xs.at[n, k, k], xr.at[n, k, k], s_xs, xp_r.at[n], dev_x(1 + 2 * k))

    piece_z = tok // n_z

    def at_z(d):
        return lax.rem(t + d + n_z, n_z)

    mid = part // 2

    def lane_half(h):
        return slice(h * mid, (h + 1) * mid)

    def z_scatter(n):
        got(PDr.at[0, n], pd_r.at[0, n])
        got(xr.at[n], xp_r.at[n])
        for h in range(2):
            total = summed(0, n, h) + xr[n, 0, h].astype(F32) + xr[n, 1, h].astype(F32)
            total = total.reshape(n_z // 2, piece_z, part)
            at = pl.ds(h * (n_z // 2), n_z // 2)
            Zt[n, at] = total
            Zs[n, at] = total.astype(BF16)
        for k in range(2):
            far = at_z(3 - 6 * k)
            send(Zs.at[n, far], Z3.at[n, k, :, 0:part], s_z, z1_r.at[n, k], dev_z(2 + (n_z - 4) * k))
            src = Zs.at[n, at_z(4), :, lane_half(k)]
            send(src, Z3.at[n, k, :, part:], s_z, z1_r.at[n, k], dev_z(2 + (n_z - 4) * k))

    def z_middle(n):
        for k in range(2):
            sign = 1 - 2 * k
            got(Z3.at[n, k], z1_r.at[n, k])
            Zm[n, 0, k] = (Zt[n, at_z(sign)] + Z3[n, k, :, 0:part].astype(F32)).astype(BF16)
            send(Zm.at[n, 0, k], Zr.at[n, 0, k], s_z, z4_r.at[n], dev_z((sign + n_z) % n_z))
            here, there = lane_half(k), lane_half(1 - k)
            next_but_one = at_z(2 * sign)
            Zm[n, 1, k, :, here] = (Zt[n, next_but_one, :, here] + Z3[n, k, :, part:].astype(F32)).astype(BF16)
            Zm[n, 1, k, :, there] = Zt[n, next_but_one, :, there].astype(BF16)
            send(Zm.at[n, 1, k], Zr.at[n, 1, k], s_z, z4_r.at[n], dev_z((2 * sign + n_z) % n_z))

    def z_gather(n):
        done = Zt[n, t]
        got(Zr.at[n], z4_r.at[n])
        for i in range(2):
            for k in range(2):
                done += Zr[n, i, k].astype(F32)
        Zf[n, t] = done.astype(BF16)
        for i in (1, 0):
            for k in range(2):
                d = (i + 1) * (1 - 2 * k)
                sem = (zd_r if i == 0 else z2_r).at[n]
                send(Zf.at[n, t], Zf.at[n, t], s_z, sem, dev_z((d + n_z) % n_z))

    def z_relay(n):
        got(Zf.at[n, 0:2], z2_r.at[n])
        for k in range(2):
            sign = 1 - 2 * k
            src = at_z(-2 * sign)
            send(Zf.at[n, src], Zf.at[n, src], s_z, zd_r.at[n], dev_z((sign + n_z) % n_z))
            at = Zf.at[n, src, :, lane_half(k)]
            send(at, at, s_z, zd_r.at[n], dev_z((2 * sign + n_z) % n_z))

    def z_done(n):
        got(Zf.at[n, 0:5], zd_r.at[n])
        pltpu.make_async_copy(Zf.at[n], out_tok.at[:, :, n * part : (n + 1) * part], loc.at[3]).start()

    def y_first():
        weights_back(at_y(2))
        for h in range(2):
            yopp[h] = acc_half(at_y(2), h).astype(BF16)
            send(yopp.at[h], yropp.at[h], s_yo, yo_r.at[h], dev_y(1 + 2 * h))

    def y_next(k):
        h = 1 - k
        weights_back(at_y(1 + 2 * k))
        ys[k, h] = acc_half(at_y(1 + 2 * k), h).astype(BF16)
        send(ys.at[k, h], yr.at[k, h], s_ys, yp_r.at[k, h], dev_y(1 + 2 * k))

    def y_second():
        for k in range(2):
            got(yropp.at[k], yo_r.at[k])
            ys[k, k] = (acc_half(at_y(1 + 2 * k), k) + yropp[k].astype(F32)).astype(BF16)
            send(ys.at[k, k], yr.at[k, k], s_ys, yp_r.at[k, k], dev_y(1 + 2 * k))

    def x_slices():
        for h in range(2):
            for k in range(2):
                got(yr.at[k, h], yp_r.at[k, h])
            value = acc_half(y, h) + yr[0, h].astype(F32) + yr[1, h].astype(F32)
            value = value.astype(BF16)
            for k in range(SIDE):
                R[h, k] = value[:, k * lanes : (k + 1) * lanes]
            OUT[x, h] = R[h, x]
            for d in (1, 3, 2):
                send(R.at[h, at_x(d)], OUT.at[x, h], s_r, ra_r.at[0], dev_x(d))

    def weights_out():
        got(OUT.at[0:3], ra_r.at[0])
        for k in range(SIDE):
            first, rest = k * q, n_acc - cut - q
            for src, dst in (
                (OUT.at[k, 0, 0:q], out_in.at[0, first : first + q]),
                (OUT.at[k, 0, q:cut], out_in.at[1, first : first + cut - q]),
                (OUT.at[k, 1, 0:rest], out_in.at[1, first + cut - q : first + q]),
                (OUT.at[k, 1, rest:cut], out_out.at[first : first + q]),
            ):
                pltpu.make_async_copy(src, dst, loc.at[4]).start()

    got_quarter(1)
    for h in range(2):
        got(unit(y, 2, h), sf_r.at[h])
        spread(2, h)
    onward(0)
    onward(1)
    over_x(1, 0, 0)
    over_x(3, 1, 0)
    got(G.at[e, 0:3], g_r.at[0])
    send(G.at[e], G.at[e], s_gd, g_r.at[1], partner)
    onward(3)
    over_x(1, 0, 1)
    over_x(3, 1, 1)
    over_z(1, 0, 0)
    over_z(3, 1, 0)
    onward(2)
    over_x(1, 1, 0)
    over_x(3, 0, 0)
    over_z(1, 0, 1)
    over_z(3, 1, 1)
    got(W.at[0:4], wrest.at[1])
    products(0, (0, 1, 3), False)
    over_x(1, 1, 1)
    over_x(3, 0, 1)
    over_z(3, 0, 0)
    over_z(1, 1, 0)
    over_x(2, 0, 0)
    over_x(2, 1, 0)
    over_z(3, 0, 1)
    over_z(1, 1, 1)
    over_x(2, 0, 1)
    over_x(2, 1, 1)
    got(W.at[0:4], wrest.at[0])
    got(G.at[1 - e], g_r.at[1])
    forward(1)
    over_z(2, 0, 0)
    over_z(2, 1, 0)
    forward(3, 1)
    over_z(2, 0, 1)
    over_z(2, 1, 1)
    forward(0, 3)
    near, far = (1, 3), (2, 1, 3)
    tokens_back(0, near)
    tokens_back(1, near)
    x_near(0)
    forward(2, 0)
    turn(2)
    x_near(1)
    tokens_back(0, (2,))
    tokens_back(1, (2,))
    x_far(0)
    y_first()
    x_far(1)
    tokens_back(2, far)
    x_second(0)
    tokens_back(3, far)
    x_far(2)
    x_near(2)
    x_second(1)
    y_next(0)
    x_far(3)
    x_near(3)
    y_next(1)
    tokens_back(0, (0,))
    x_second(2)
    z_scatter(0)
    tokens_back(1, (0,))
    tokens_back(2, (0,))
    z_scatter(1)
    tokens_back(3, (0,))
    y_second()
    z_middle(0)
    weights_back(y)
    x_second(3)
    z_scatter(2)
    z_middle(1)
    z_gather(0)
    z_scatter(3)
    z_middle(2)
    z_gather(1)
    z_relay(0)
    z_middle(3)
    z_gather(2)
    x_slices()
    z_relay(1)
    z_gather(3)
    z_relay(2)
    z_done(0)
    z_relay(3)
    z_done(1)
    weights_out()
    z_done(2)
    z_done(3)
    for ref, sem in (
        (W, s_w), (X.at[:, :, :, 0 : tok - tok // 8, :], s_x), (PDs, s_pd), (xopp, s_xo), (xs, s_xs), (yopp, s_yo),
        (ys, s_ys), (R.at[:, 0:3], s_r), (Zt.at[:, 0:7], s_z), (G.at[0, 0:3], s_g), (G.at[0], s_gd),
    ):
        sent(ref, sem)
    got(OUT, loc.at[4])
    got(Zf, loc.at[3])


def widen_kernel(*refs):
    for src, dst in zip(refs[:3], refs[3:]):
        dst[...] = src[...].astype(F32)


def widen(tok, w_in, w_out):
    steps = 4
    specs = [
        pl.BlockSpec((tok.shape[0] // steps, tok.shape[1]), lambda i: (i, 0)),
        pl.BlockSpec((2, w_in.shape[1] // steps, w_in.shape[2]), lambda i: (0, i, 0)),
        pl.BlockSpec((w_out.shape[0] // steps, w_out.shape[1]), lambda i: (i, 0)),
    ]
    return pl.pallas_call(
        widen_kernel,
        grid=(steps,),
        in_specs=specs,
        out_specs=specs,
        out_shape=[jax.ShapeDtypeStruct(a.shape, F32) for a in (tok, w_in, w_out)],
    )(tok, w_in, w_out)


def shards(n_z, tokens, tangent, cotangent, expert_ids, gates, w_in, v_in, w_out, v_out):
    tok = tokens.shape[0]
    ff, lanes = w_in.shape[2:]
    width = tokens.shape[1]
    q = ff // SIDE
    half = tok // 2
    part = width // SIDE
    cut = 3 * q // 2
    dma = pltpu.SemaphoreType.DMA
    vmem = pl.BlockSpec(memory_space=pltpu.VMEM)
    hbm = pl.BlockSpec(memory_space=pltpu.HBM)
    y_tok, y_in, y_out = pl.pallas_call(
        functools.partial(kernel, n_z),
        out_shape=(
            jax.ShapeDtypeStruct((n_z, tok // n_z, width), BF16),
            jax.ShapeDtypeStruct((2, ff, lanes), BF16),
            jax.ShapeDtypeStruct((ff, lanes), BF16),
        ),
        in_specs=[vmem, vmem] + [hbm] * 7,
        out_specs=(hbm, hbm, hbm),
        scratch_shapes=[
            pltpu.VMEM((SIDE * SIDE, 6, q, lanes), BF16),
            pltpu.VMEM((6, ff, lanes), BF16),
            pltpu.VMEM((2, 3, q, lanes), BF16),
            pltpu.VMEM((3, SIDE, 2, tok, width), BF16),
            pltpu.VMEM((2, SIDE, 8, tok), F32),
            pltpu.VMEM((4, 8 * q, 2 * tok), F32),
            pltpu.VMEM((4 * q, SIDE * 2 * tok), BF16),
            pltpu.VMEM((4, 2 * tok, 4 * q), BF16),
            pltpu.VMEM((q, SIDE * 2 * tok), BF16),
            pltpu.VMEM((SIDE, 3 * q, part), F32),
            pltpu.VMEM((4, SIDE, tok, part), F32),
            pltpu.VMEM((4, SIDE, tok, part), BF16),
            pltpu.VMEM((4, SIDE, tok, part), BF16),
            pltpu.VMEM((SIDE, 2, 2, half, part), BF16),
            pltpu.VMEM((SIDE, 2, half, part), BF16),
            pltpu.VMEM((SIDE, 2, 2, half, part), BF16),
            pltpu.VMEM((SIDE, 2, half, part), BF16),
            pltpu.VMEM((2, 2, cut, part), BF16),
            pltpu.VMEM((2, cut, part), BF16),
            pltpu.VMEM((2, 2, cut, part), BF16),
            pltpu.VMEM((2, cut, part), BF16),
            pltpu.VMEM((2, SIDE, cut, lanes), BF16),
            pltpu.VMEM((SIDE, 2, cut, lanes), BF16),
            pltpu.VMEM((SIDE, n_z, tok // n_z, part), F32),
            pltpu.VMEM((SIDE, n_z, tok // n_z, part), BF16),
            pltpu.VMEM((SIDE, 2, tok // n_z, part + part // 2), BF16),
            pltpu.VMEM((SIDE, 2, 2, tok // n_z, part), BF16),
            pltpu.VMEM((SIDE, 2, 2, tok // n_z, part), BF16),
            pltpu.VMEM((SIDE, n_z, tok // n_z, part), BF16),
            dma((5,)),
            dma((11,)),
            dma((2, 2)), dma((2,)), dma((2,)),
            dma((2, 4)), dma((2,)),
            dma((2, 2, 2)), dma((2, 2)), dma((3, 2, 2)),
            dma((2,)), dma((4,)), dma((4, 4)),
            dma((4, 2)), dma((4,)),
            dma((2,)), dma((2, 2)), dma((1,)),
            dma((4, 2)), dma((4,)), dma((4,)), dma((4,)),
        ],
        compiler_params=pltpu.CompilerParams(
            collective_id=0, has_side_effects=True, vmem_limit_bytes=62 * 1024 * 1024
        ),
    )(
        expert_ids.T, gates.T, tokens, tangent, cotangent, w_in[0], v_in[0], w_out[0], v_out[0]
    )
    y_tok, y_in, y_out = widen(y_tok.reshape(tok, width), y_in, y_out)
    return y_tok, y_in[None], y_out[None]


def solution(mesh):
    rows = P(("expert", "dp"), None)
    w_spec = P(("tensor", "expert"), None, None, "dp")
    o_spec = P(("tensor", "expert"), None, "dp")
    return jax.shard_map(
        functools.partial(shards, mesh.shape["tensor"]),
        mesh=mesh,
        in_specs=(rows,) * 5 + (w_spec, w_spec, o_spec, o_spec),
        out_specs=(rows, w_spec, o_spec),
        check_vma=False,
    )
```

```python
import functools

import jax
import jax.numpy as jnp
from jax import lax
from jax.experimental import pallas as pl
from jax.experimental.pallas import tpu as pltpu
from jax.sharding import PartitionSpec as P

MESH = pl.DeviceIdType.MESH
F32 = jnp.float32
BF16 = jnp.bfloat16
SIDE = 4
NT = (((1,), (1,)), ((), ()))
NN = (((1,), (0,)), ((), ()))


def mm(a, b, dims=NN):
    return lax.dot_general(a, b, dims, preferred_element_type=F32)


def kernel(
    n_z, ids_ref, gates_ref, tok_ref, tan_ref, cot_ref, wi_ref, vi_ref, wo_ref, vo_ref,
    out_tok, out_in, out_out,
    W, Wsrc, stage, X, G, C, S, ST, H, acc, Pown, PDs, PDr, xs, xopp, xr, xropp, ys, yopp, yr, yropp, R, OUT, Zt, Zs, Z3, Zm, Zr, Zf,
    loc, snd, wa_r, st_r, sf_r, wy_r, wrest, xh_r, xf_r, zx_r, g_r, dd_r, pd_r, xo_r, xp_r, yo_r, yp_r, ra_r,
    z1_r, z4_r, z2_r, zd_r,
):
    t = lax.axis_index("tensor")
    e = lax.axis_index("expert")
    p = lax.axis_index("dp")
    y, x = p // SIDE, p % SIDE
    color = lax.rem(t, 2)
    tok = tok_ref.shape[0]
    half = tok // 2
    quarter = tok // 4
    lanes = wi_ref.shape[-1]
    q = W.shape[2]
    width = tok_ref.shape[1]
    part = width // SIDE

    def at_x(d):
        return lax.rem(x + d, SIDE)

    def at_y(d):
        return lax.rem(y + d, SIDE)

    def dev_x(d):
        return (t, e, y * SIDE + at_x(d))

    def dev_y(d):
        return (t, e, at_y(d) * SIDE + x)

    def dev_z(d):
        return (lax.rem(t + d, n_z), e, p)

    partner = (t, 1 - e, p)
    s_w, s_x, s_pd, s_xo, s_xs, s_yo, s_ys, s_r, s_z, s_g, s_gd = (snd.at[i] for i in range(11))

    def send(src, dst, ssem, rsem, dev):
        pltpu.make_async_remote_copy(
            src_ref=src, dst_ref=dst, send_sem=ssem, recv_sem=rsem, device_id=dev, device_id_type=MESH
        ).start()

    def got(ref, rsem):
        pltpu.make_async_remote_copy(
            src_ref=ref, dst_ref=ref, send_sem=s_w, recv_sem=rsem, device_id=partner, device_id_type=MESH
        ).wait_recv()

    def sent(ref, ssem):
        pltpu.make_async_remote_copy(
            src_ref=ref, dst_ref=ref, send_sem=ssem, recv_sem=ssem, device_id=partner, device_id_type=MESH
        ).wait_send()

    barrier = pltpu.get_barrier_semaphore()
    peers = [partner] + [dev_x(d) for d in (1, 2, 3)] + [dev_y(d) for d in (1, 3)] + [dev_z(d) for d in (1, 2, n_z - 2, n_z - 1)]
    for peer in peers:
        pl.semaphore_signal(barrier, inc=1, device_id=peer, device_id_type=MESH)

    def rows(k):
        return pl.ds(pl.multiple_of(k * q, q), q)

    for src, dst, i in (
        (wi_ref, Wsrc.at[0:2], 0),
        (wo_ref, Wsrc.at[2], 0),
        (vi_ref, Wsrc.at[3:5], 0),
        (vo_ref, Wsrc.at[5], 0),
        (wi_ref.at[:, rows(x), :], W.at[p, 0:2], 1),
        (wo_ref.at[rows(x), :], W.at[p, 2], 1),
        (vi_ref.at[:, rows(x), :], W.at[p, 3:5], 1),
        (vo_ref.at[rows(x), :], W.at[p, 5], 1),
        (tok_ref, X.at[0, x, e], 2),
        (tan_ref, X.at[1, x, e], 2),
        (cot_ref, X.at[2, x, e], 2),
    ):
        pltpu.make_async_copy(src, dst, loc.at[i]).start()
    ids, gates = ids_ref[...], gates_ref[...]
    for r in range(2):
        G[e, x, pl.ds(r, 1), :] = jnp.sum(jnp.where(ids == 2 * t + r, gates, 0.0), axis=0, keepdims=True)
    pl.semaphore_wait(barrier, len(peers))

    got(Wsrc, loc.at[0])

    def quarter_of(h, k):
        return Wsrc.at[3 * h : 3 * h + 3, rows(k), :]

    def unit(yy, d, h):
        return W.at[yy * SIDE + at_x(SIDE - d), 3 * h : 3 * h + 3]

    def quarter_to(h):
        for k, d in enumerate((1, 3)):
            send(quarter_of(h, at_x(d)), unit(y, 0, h), s_w, wa_r.at[k, h], dev_x(d))

    quarter_to(0)
    for h in range(2):
        send(quarter_of(h, at_x(2)), stage.at[h], s_w, st_r.at[h], dev_x(1 + 2 * h))
    quarter_to(1)
    for d in (1, 3, 2):
        send(G.at[e, x], G.at[e, x], s_g, g_r.at[0], dev_x(d))
    got(W.at[p], loc.at[1])

    order = (0, 1, 3, 2)

    def spread(d, h):
        k = order.index(d)
        for i in range(2):
            sem = wy_r.at[i, k] if i == h else wrest.at[1]
            send(unit(y, d, h), unit(y, d, h), s_w, sem, dev_y(1 + 2 * i))

    def onward(d):
        k = order.index(d)
        for h in range(2):
            at = unit(at_y(3 - 2 * h), d, h)
            got(at, wy_r.at[h, k])
            send(at, at, s_w, wrest.at[0], dev_y(1 + 2 * h))

    def got_quarter(h):
        for k, d in enumerate((1, 3)):
            got(unit(y, d, h), wa_r.at[k, h])
            spread(d, h)

    spread(0, 0)
    spread(0, 1)
    got(X.at[:, x, e], loc.at[2])

    def piece(a, own, h, i):
        eighth = quarter // 2
        first = (color if own else 1 - color) * half + h * quarter + i * eighth
        return X.at[:, a, e, pl.ds(pl.multiple_of(first, eighth), eighth), :]

    def over_links(k, h, i):
        at = piece(x, True, h, i)
        send(at, at, s_x, xh_r.at[k, h, i], dev_x(1 + 2 * k))

    over_links(0, 0, 0)
    over_links(1, 1, 0)
    send(X.at[:, x, e], X.at[:, x, e], s_x, dd_r.at[0], partner)
    got_quarter(0)
    for h in range(2):
        got(stage.at[h], st_r.at[h])
        send(stage.at[h], unit(y, 1 + 2 * h, h), s_w, sf_r.at[h], dev_x(1 + 2 * h))
    for k, h, i in ((0, 0, 1), (1, 1, 1), (0, 1, 0), (1, 0, 0), (0, 1, 1), (1, 0, 1)):
        over_links(k, h, i)

    def over_x(rel, h, i):
        at = piece(at_x(SIDE - rel), True, h, i)
        if rel == 2:
            got(at, xf_r.at[h, i])
        else:
            k = rel // 2
            got(at, xh_r.at[k, h, i])
            if h == k:
                send(at, at, s_x, xf_r.at[h, i], dev_x(1 + 2 * k))
        send(at, at, s_x, zx_r.at[rel - 1, h, i], dev_z(1 if h == 0 else n_z - 1))
        send(at, at, s_x, dd_r.at[rel], partner)

    def over_z(rel, h, i):
        at = piece(at_x(SIDE - rel), False, h, i)
        got(at, zx_r.at[rel - 1, h, i])
        send(at, at, s_x, dd_r.at[rel], partner)

    n_acc = acc.shape[1]
    cut = n_acc // 2
    step = 32

    def tokens_of(a):
        return pl.ds(pl.multiple_of(a * 2 * tok, 2 * tok), 2 * tok)

    def weights(lo, hi, slabs=range(SIDE * SIDE)):
        return jnp.concatenate([W[k, lo:hi].reshape((hi - lo) * q, lanes) for k in slabs], axis=1)

    def turn(rel):
        ST[rel] = S[:, tokens_of(at_x(SIDE - rel))].T

    def products(rel, quarters, add):
        a = at_x(SIDE - rel)
        if not add:
            got(X.at[:, a, 1 - e], dd_r.at[rel])
        slabs = [at_y(d) * SIDE + k for d in quarters for k in range(SIDE)]
        for first, lo, hi, i in ((0, 0, 2, 0), (2, 3, 5, 0), (4, 0, 2, 1), (6, 2, 3, 2), (7, 5, 6, 2)):
            cols = [pl.ds(pl.multiple_of(at_y(d) * part, part), part) for d in quarters]
            right = jnp.concatenate([X[i, a, :, :, c].reshape(2 * tok, part) for c in cols], axis=1)
            value = mm(weights(lo, hi, slabs), right, NT)
            at = slice(first * q, (first + hi - lo) * q)
            C[rel, at, :] = C[rel, at, :] + value if add else value

    def forward(rel, before=None):
        a = at_x(SIDE - rel)
        if before is not None:
            turn(before)
        products(rel, (2,) if rel == 0 else (0, 1, 3, 2), rel == 0)
        gate = jnp.concatenate([G[0, a, pl.ds(e, 1), :], G[1, a, pl.ds(e, 1), :]], axis=1)
        cols = tokens_of(a)

        def rows_of(i, carry):
            at = pl.multiple_of(i * step, step)

            def c(k):
                return C[rel, pl.ds(k * q + at, step), :]

            pre, up = c(0), c(1)
            pre_dot, up_dot = c(4) + c(2), c(5) + c(3)
            g, g_dot = c(6) * gate, c(7) * gate
            sigma = jax.nn.sigmoid(pre)
            rest = 1.0 - sigma
            s0 = pre * sigma
            s1 = sigma * (1.0 + pre * rest)
            s2 = sigma * rest * (2.0 + pre * (1.0 - 2.0 * sigma))
            S[pl.ds(at, step), cols] = (
                g_dot * up * s1 + g * up_dot * s1 + g * up * s2 * pre_dot
            ).astype(BF16)
            S[pl.ds(q + at, step), cols] = (g_dot * s0 + g * s1 * pre_dot).astype(BF16)
            S[pl.ds(2 * q + at, step), cols] = (g * up * s1).astype(BF16)
            S[pl.ds(3 * q + at, step), cols] = (g * s0).astype(BF16)
            H[pl.ds(at, step), cols] = ((s1 * pre_dot * up + s0 * up_dot) * gate).astype(BF16)
            return carry

        lax.fori_loop(0, q // step, rows_of, 0)

    def tokens_back(n, rels):
        slabs = range(SIDE * n, SIDE * n + SIDE)
        for rel in rels:
            left = jnp.concatenate(
                [ST[rel, pl.ds(pl.multiple_of(k * tok, tok), tok), :] for k in (e, 1 - e)], axis=0
            )
            value = mm(left[:, 0 : 2 * q], weights(0, 2, slabs)) + mm(left[:, 2 * q : 4 * q], weights(3, 5, slabs))
            Pown[rel, n] = value[0:tok]
            PDs[rel, n] = value[tok : 2 * tok].astype(BF16)
            send(PDs.at[rel, n], PDr.at[rel, n], s_pd, pd_r.at[rel, n], partner)

    def weights_back(n):
        cols = pl.ds(pl.multiple_of(n * part, part), part)

        def every(i):
            return X[i, :, :, :, cols].reshape(SIDE * 2 * tok, part)

        acc[n, 0 : 2 * q, :] = mm(S[2 * q : 4 * q, :], every(1)) + mm(S[0 : 2 * q, :], every(0))
        acc[n, 2 * q : 3 * q, :] = mm(H[...], every(2))

    def summed(rel, n, h):
        at = pl.ds(h * half, half)
        return Pown[rel, n, at, :] + PDr[rel, n, at, :].astype(F32)

    def acc_half(k, h):
        return acc[k, h * cut : (h + 1) * cut, :]

    def x_far(n):
        got(PDr.at[2, n], pd_r.at[2, n])
        for h in range(2):
            xopp[n, h] = summed(2, n, h).astype(BF16)
            send(xopp.at[n, h], xropp.at[n, h], s_xo, xo_r.at[n, h], dev_x(1 + 2 * h))

    def x_near(n):
        for rel, k, h in ((1, 1, 0), (3, 0, 1)):
            got(PDr.at[rel, n], pd_r.at[rel, n])
            xs[n, k, h] = summed(rel, n, h).astype(BF16)
            send(xs.at[n, k, h], xr.at[n, k, h], s_xs, xp_r.at[n], dev_x(1 + 2 * k))

    def x_second(n):
        for k in range(2):
            got(xropp.at[n, k], xo_r.at[n, k])
            xs[n, k, k] = (summed(3 - 2 * k, n, k) + xropp[n, k].astype(F32)).astype(BF16)
            send(xs.at[n, k, k], xr.at[n, k, k], s_xs, xp_r.at[n], dev_x(1 + 2 * k))

    piece_z = tok // n_z

    def at_z(d):
        return lax.rem(t + d + n_z, n_z)

    mid = part // 2

    def lane_half(h):
        return slice(h * mid, (h + 1) * mid)

    def z_scatter(n):
        got(PDr.at[0, n], pd_r.at[0, n])
        got(xr.at[n], xp_r.at[n])
        for h in range(2):
            total = summed(0, n, h) + xr[n, 0, h].astype(F32) + xr[n, 1, h].astype(F32)
            total = total.reshape(n_z // 2, piece_z, part)
            at = pl.ds(h * (n_z // 2), n_z // 2)
            Zt[n, at] = total
            Zs[n, at] = total.astype(BF16)
        for k in range(2):
            far = at_z(3 - 6 * k)
            send(Zs.at[n, far], Z3.at[n, k, :, 0:part], s_z, z1_r.at[n, k], dev_z(2 + (n_z - 4) * k))
            src = Zs.at[n, at_z(4), :, lane_half(k)]
            send(src, Z3.at[n, k, :, part:], s_z, z1_r.at[n, k], dev_z(2 + (n_z - 4) * k))

    def z_middle(n):
        for k in range(2):
            sign = 1 - 2 * k
            got(Z3.at[n, k], z1_r.at[n, k])
            Zm[n, 0, k] = (Zt[n, at_z(sign)] + Z3[n, k, :, 0:part].astype(F32)).astype(BF16)
            send(Zm.at[n, 0, k], Zr.at[n, 0, k], s_z, z4_r.at[n], dev_z((sign + n_z) % n_z))
            here, there = lane_half(k), lane_half(1 - k)
            next_but_one = at_z(2 * sign)
            Zm[n, 1, k, :, here] = (Zt[n, next_but_one, :, here] + Z3[n, k, :, part:].astype(F32)).astype(BF16)
            Zm[n, 1, k, :, there] = Zt[n, next_but_one, :, there].astype(BF16)
            send(Zm.at[n, 1, k], Zr.at[n, 1, k], s_z, z4_r.at[n], dev_z((2 * sign + n_z) % n_z))

    def z_gather(n):
        done = Zt[n, t]
        got(Zr.at[n], z4_r.at[n])
        for i in range(2):
            for k in range(2):
                done += Zr[n, i, k].astype(F32)
        Zf[n, t] = done.astype(BF16)
        for i in (1, 0):
            for k in range(2):
                d = (i + 1) * (1 - 2 * k)
                sem = (zd_r if i == 0 else z2_r).at[n]
                send(Zf.at[n, t], Zf.at[n, t], s_z, sem, dev_z((d + n_z) % n_z))

    def z_relay(n):
        got(Zf.at[n, 0:2], z2_r.at[n])
        for k in range(2):
            sign = 1 - 2 * k
            src = at_z(-2 * sign)
            send(Zf.at[n, src], Zf.at[n, src], s_z, zd_r.at[n], dev_z((sign + n_z) % n_z))
            at = Zf.at[n, src, :, lane_half(k)]
            send(at, at, s_z, zd_r.at[n], dev_z((2 * sign + n_z) % n_z))

    def z_done(n):
        got(Zf.at[n, 0:5], zd_r.at[n])
        pltpu.make_async_copy(Zf.at[n], out_tok.at[:, :, n * part : (n + 1) * part], loc.at[3]).start()

    def y_first():
        weights_back(at_y(2))
        for h in range(2):
            yopp[h] = acc_half(at_y(2), h).astype(BF16)
            send(yopp.at[h], yropp.at[h], s_yo, yo_r.at[h], dev_y(1 + 2 * h))

    def y_next(k):
        h = 1 - k
        weights_back(at_y(1 + 2 * k))
        ys[k, h] = acc_half(at_y(1 + 2 * k), h).astype(BF16)
        send(ys.at[k, h], yr.at[k, h], s_ys, yp_r.at[k, h], dev_y(1 + 2 * k))

    def y_second():
        for k in range(2):
            got(yropp.at[k], yo_r.at[k])
            ys[k, k] = (acc_half(at_y(1 + 2 * k), k) + yropp[k].astype(F32)).astype(BF16)
            send(ys.at[k, k], yr.at[k, k], s_ys, yp_r.at[k, k], dev_y(1 + 2 * k))

    def x_slices():
        for h in range(2):
            for k in range(2):
                got(yr.at[k, h], yp_r.at[k, h])
            value = acc_half(y, h) + yr[0, h].astype(F32) + yr[1, h].astype(F32)
            value = value.astype(BF16)
            for k in range(SIDE):
                R[h, k] = value[:, k * lanes : (k + 1) * lanes]
            OUT[x, h] = R[h, x]
            for d in (1, 3, 2):
                send(R.at[h, at_x(d)], OUT.at[x, h], s_r, ra_r.at[0], dev_x(d))

    def weights_out():
        got(OUT.at[0:3], ra_r.at[0])
        for k in range(SIDE):
            first, rest = k * q, n_acc - cut - q
            for src, dst in (
                (OUT.at[k, 0, 0:q], out_in.at[0, first : first + q]),
                (OUT.at[k, 0, q:cut], out_in.at[1, first : first + cut - q]),
                (OUT.at[k, 1, 0:rest], out_in.at[1, first + cut - q : first + q]),
                (OUT.at[k, 1, rest:cut], out_out.at[first : first + q]),
            ):
                pltpu.make_async_copy(src, dst, loc.at[4]).start()

    got_quarter(1)
    for h in range(2):
        got(unit(y, 2, h), sf_r.at[h])
        spread(2, h)
    onward(0)
    onward(1)
    over_x(1, 0, 0)
    over_x(3, 1, 0)
    got(G.at[e, 0:3], g_r.at[0])
    send(G.at[e], G.at[e], s_gd, g_r.at[1], partner)
    onward(3)
    over_x(1, 0, 1)
    over_x(3, 1, 1)
    over_z(1, 0, 0)
    over_z(3, 1, 0)
    onward(2)
    over_x(1, 1, 0)
    over_x(3, 0, 0)
    over_z(1, 0, 1)
    over_z(3, 1, 1)
    got(W.at[0:4], wrest.at[1])
    products(0, (0, 1, 3), False)
    over_x(1, 1, 1)
    over_x(3, 0, 1)
    over_z(3, 0, 0)
    over_z(1, 1, 0)
    over_x(2, 0, 0)
    over_x(2, 1, 0)
    over_z(3, 0, 1)
    over_z(1, 1, 1)
    over_x(2, 0, 1)
    over_x(2, 1, 1)
    got(W.at[0:4], wrest.at[0])
    got(G.at[1 - e], g_r.at[1])
    forward(1)
    over_z(2, 0, 0)
    over_z(2, 1, 0)
    forward(3, 1)
    over_z(2, 0, 1)
    over_z(2, 1, 1)
    forward(0, 3)
    near, far = (1, 3), (2, 1, 3)
    tokens_back(0, near)
    tokens_back(1, near)
    x_near(0)
    forward(2, 0)
    turn(2)
    x_near(1)
    tokens_back(0, (2,))
    tokens_back(1, (2,))
    x_far(0)
    y_first()
    x_far(1)
    tokens_back(2, far)
    x_second(0)
    tokens_back(3, far)
    x_far(2)
    x_near(2)
    x_second(1)
    y_next(0)
    x_far(3)
    x_near(3)
    y_next(1)
    tokens_back(0, (0,))
    x_second(2)
    z_scatter(0)
    tokens_back(1, (0,))
    tokens_back(2, (0,))
    z_scatter(1)
    tokens_back(3, (0,))
    y_second()
    z_middle(0)
    weights_back(y)
    x_second(3)
    z_scatter(2)
    z_middle(1)
    z_gather(0)
    z_scatter(3)
    z_middle(2)
    z_gather(1)
    z_relay(0)
    z_middle(3)
    z_gather(2)
    x_slices()
    z_relay(1)
    z_gather(3)
    z_relay(2)
    z_done(0)
    z_relay(3)
    z_done(1)
    weights_out()
    z_done(2)
    z_done(3)
    for ref, sem in (
        (W, s_w), (X.at[:, :, :, 0 : tok - tok // 8, :], s_x), (PDs, s_pd), (xopp, s_xo), (xs, s_xs), (yopp, s_yo),
        (ys, s_ys), (R.at[:, 0:3], s_r), (Zt.at[:, 0:7], s_z), (G.at[0, 0:3], s_g), (G.at[0], s_gd),
    ):
        sent(ref, sem)
    got(OUT, loc.at[4])
    got(Zf, loc.at[3])


def widen_kernel(*refs):
    for src, dst in zip(refs[:3], refs[3:]):
        dst[...] = src[...].astype(F32)


def widen(tok, w_in, w_out):
    steps = 1
    specs = [
        pl.BlockSpec((tok.shape[0] // steps, tok.shape[1]), lambda i: (i, 0)),
        pl.BlockSpec((2, w_in.shape[1] // steps, w_in.shape[2]), lambda i: (0, i, 0)),
        pl.BlockSpec((w_out.shape[0] // steps, w_out.shape[1]), lambda i: (i, 0)),
    ]
    return pl.pallas_call(
        widen_kernel,
        grid=(steps,),
        in_specs=specs,
        out_specs=specs,
        out_shape=[jax.ShapeDtypeStruct(a.shape, F32) for a in (tok, w_in, w_out)],
    )(tok, w_in, w_out)


def shards(n_z, tokens, tangent, cotangent, expert_ids, gates, w_in, v_in, w_out, v_out):
    tok = tokens.shape[0]
    ff, lanes = w_in.shape[2:]
    width = tokens.shape[1]
    q = ff // SIDE
    half = tok // 2
    part = width // SIDE
    cut = 3 * q // 2
    dma = pltpu.SemaphoreType.DMA
    vmem = pl.BlockSpec(memory_space=pltpu.VMEM)
    hbm = pl.BlockSpec(memory_space=pltpu.HBM)
    y_tok, y_in, y_out = pl.pallas_call(
        functools.partial(kernel, n_z),
        out_shape=(
            jax.ShapeDtypeStruct((n_z, tok // n_z, width), BF16),
            jax.ShapeDtypeStruct((2, ff, lanes), BF16),
            jax.ShapeDtypeStruct((ff, lanes), BF16),
        ),
        in_specs=[vmem, vmem] + [hbm] * 7,
        out_specs=(hbm, hbm, hbm),
        scratch_shapes=[
            pltpu.VMEM((SIDE * SIDE, 6, q, lanes), BF16),
            pltpu.VMEM((6, ff, lanes), BF16),
            pltpu.VMEM((2, 3, q, lanes), BF16),
            pltpu.VMEM((3, SIDE, 2, tok, width), BF16),
            pltpu.VMEM((2, SIDE, 8, tok), F32),
            pltpu.VMEM((4, 8 * q, 2 * tok), F32),
            pltpu.VMEM((4 * q, SIDE * 2 * tok), BF16),
            pltpu.VMEM((4, 2 * tok, 4 * q), BF16),
            pltpu.VMEM((q, SIDE * 2 * tok), BF16),
            pltpu.VMEM((SIDE, 3 * q, part), F32),
            pltpu.VMEM((4, SIDE, tok, part), F32),
            pltpu.VMEM((4, SIDE, tok, part), BF16),
            pltpu.VMEM((4, SIDE, tok, part), BF16),
            pltpu.VMEM((SIDE, 2, 2, half, part), BF16),
            pltpu.VMEM((SIDE, 2, half, part), BF16),
            pltpu.VMEM((SIDE, 2, 2, half, part), BF16),
            pltpu.VMEM((SIDE, 2, half, part), BF16),
            pltpu.VMEM((2, 2, cut, part), BF16),
            pltpu.VMEM((2, cut, part), BF16),
            pltpu.VMEM((2, 2, cut, part), BF16),
            pltpu.VMEM((2, cut, part), BF16),
            pltpu.VMEM((2, SIDE, cut, lanes), BF16),
            pltpu.VMEM((SIDE, 2, cut, lanes), BF16),
            pltpu.VMEM((SIDE, n_z, tok // n_z, part), F32),
            pltpu.VMEM((SIDE, n_z, tok // n_z, part), BF16),
            pltpu.VMEM((SIDE, 2, tok // n_z, part + part // 2), BF16),
            pltpu.VMEM((SIDE, 2, 2, tok // n_z, part), BF16),
            pltpu.VMEM((SIDE, 2, 2, tok // n_z, part), BF16),
            pltpu.VMEM((SIDE, n_z, tok // n_z, part), BF16),
            dma((5,)),
            dma((11,)),
            dma((2, 2)), dma((2,)), dma((2,)),
            dma((2, 4)), dma((2,)),
            dma((2, 2, 2)), dma((2, 2)), dma((3, 2, 2)),
            dma((2,)), dma((4,)), dma((4, 4)),
            dma((4, 2)), dma((4,)),
            dma((2,)), dma((2, 2)), dma((1,)),
            dma((4, 2)), dma((4,)), dma((4,)), dma((4,)),
        ],
        compiler_params=pltpu.CompilerParams(
            collective_id=0, has_side_effects=True, vmem_limit_bytes=62 * 1024 * 1024
        ),
    )(
        expert_ids.T, gates.T, tokens, tangent, cotangent, w_in[0], v_in[0], w_out[0], v_out[0]
    )
    y_tok, y_in, y_out = widen(y_tok.reshape(tok, width), y_in, y_out)
    return y_tok, y_in[None], y_out[None]


def solution(mesh):
    rows = P(("expert", "dp"), None)
    w_spec = P(("tensor", "expert"), None, None, "dp")
    o_spec = P(("tensor", "expert"), None, "dp")
    return jax.shard_map(
        functools.partial(shards, mesh.shape["tensor"]),
        mesh=mesh,
        in_specs=(rows,) * 5 + (w_spec, w_spec, o_spec, o_spec),
        out_specs=(rows, w_spec, o_spec),
        check_vma=False,
    )
```
